512 devices in a mesh: row: 32 (over x_lo, z, core), col: 16 (over x_hi, y).
Axes of the slice: x: 4 (x_hi: 2, x_lo: 2; x = x_hi * 2 + x_lo), y: 8, z: 8, core: 2. Of those that a mesh axis runs over, the one named last changes fastest.
Arguments:
- starting_state: float32 [65536, 256], P(('row', 'col')), may hold values from -1 to 1
- features: float32 [65536, 128], P(('row', 'col')), may hold values from -6 to 6
- cotangent: float32 [65536, 256], P(('row', 'col')), may hold values from -6 to 6
- degrees: int32 [65536], P(('row', 'col')), may hold values from 8 to 64
- tile_values: bfloat16 [32, 16, 64, 128, 128], P('row', 'col'), may hold values from 0 to 1, as said below
- tile_rows: int32 [32, 16, 64], P('row', 'col'), may hold values from 0 to 15, as said below
- tile_cols: int32 [32, 16, 64], P('row', 'col'), may hold values from 0 to 31, as said below
- tile_live: int32 [32, 16, 64], P('row', 'col'), may hold values from 0 to 1, as said below
- weight: float32 [256, 256], replicated, may hold values from -0.375 to 0.375
- input_map: float32 [128, 256], replicated, may hold values from -0.5 to 0.5
Outputs:
- states: float32 [65536, 256], P(('row', 'col'))
- adjoint: float32 [65536, 256], P(('row', 'col'))
- weight_grad: float32 [256, 256], replicated
- input_grad: float32 [128, 256], replicated
The draws below stay inside these ranges and needn't reach their ends.
Inputs may be any that keep to these rules, and one draw needn't show every extreme that they name: `tile_rows`: together with tile_cols, the slots of one device name distinct tiles. `tile_cols`: together with tile_rows, the slots of one device name distinct tiles. `tile_live`: on each device the live slots come first; every device has at least a quarter of its 64 slots live (and at least one), and some device has all 64 live. `tile_values`: roughly half of the entries of each tile are nonzero; nonzero weights lie in (0, 1].
All inputs are finite; a program needn't handle non-finite values.
Results may differ from the reference program's by a relative error of at most 0.012.
Values may be sent and summed in bfloat16 or wider, within the bound.
No kernel may reach another device: no remote copies, remote signals or barrier semaphores. Data moves between devices by JAX's collectives and lax.ppermute only.
A program may use at most 64 MiB of HBM per device.

```python
import math
import jax
import jax.numpy as jnp
from jax import lax

WIDTH = 256
INPUTS = 128
BLOCK = 128
NODE_DEV = 128
ITERS = 1
NODES = 65536
TILE_ROWS = 16
TILE_COLS = 32
SLOTS = 64
N_ROW = 32
N_COL = 16


def tile_places(key):
    base = jax.random.fold_in(key, 101)
    keys = jax.random.split(base, N_ROW * N_COL)

    def one_device(device_key):
        return jax.random.permutation(device_key, TILE_ROWS * TILE_COLS)[:SLOTS]
    places = jax.vmap(one_device)(keys)
    return places.reshape(N_ROW, N_COL, SLOTS).astype(jnp.int32)


def draw_tile_rows(key, part):
    return (tile_places(key) // TILE_COLS).astype(jnp.int32)


def draw_tile_cols(key, part):
    return (tile_places(key) % TILE_COLS).astype(jnp.int32)


def draw_tile_live(key, part):
    base = jax.random.fold_in(key, 202)
    lowest = max(1, SLOTS // 4)
    first = jax.random.randint(base, (N_ROW * N_COL,), lowest, SLOTS + 1)
    second = jax.random.randint(jax.random.fold_in(base, 7), (N_ROW * N_COL,), lowest, SLOTS + 1)
    counts = jnp.minimum(first, second)
    chosen = jax.random.randint(jax.random.fold_in(base, 1), (), 0, N_ROW * N_COL)
    counts = jnp.where(jnp.arange(N_ROW * N_COL) == chosen, SLOTS, counts)
    live = (jnp.arange(SLOTS)[None, :] < counts[:, None]).astype(jnp.int32)
    return live.reshape(N_ROW, N_COL, SLOTS)


def draw_tile_values(key, part):
    base = jax.random.fold_in(key, 303)
    random_key_length, key_keep = jax.random.split(base, 2)
    shape = (N_ROW, N_COL, SLOTS, BLOCK, BLOCK)
    sizes_drawn = jnp.exp(jax.random.uniform(random_key_length, shape, jnp.float32, jnp.log(0.1), 0.0))
    keeping = jax.random.uniform(key_keep, shape, jnp.float32) < 0.5
    return jnp.where(keeping, sizes_drawn, 0.0).astype(jnp.bfloat16)


def with_ends(array, key, smallest, largest):
    shape = array.shape
    spot = [jax.random.randint(jax.random.fold_in(key, axis), (), 0, shape[axis]) for axis in range(len(shape))]
    array = array.at[tuple(spot)].set(smallest)
    longest = shape.index(max(shape))
    spot[longest] = (spot[longest] + 1) % shape[longest]
    return array.at[tuple(spot)].set(largest)


def shard_levels(stream_key, extent, shards, least, largest):
    def one(dim, shards_of):
        steps = jax.random.uniform(jax.random.fold_in(jax.random.fold_in(stream_key, 6), dim), (shards_of,), jnp.float32, least / len(shards), largest / len(shards))
        return jnp.repeat(jnp.exp(steps), extent[dim] // shards_of).reshape((-1,) + (1,) * (len(extent) - dim - 1))

    factor_of = one(*shards[0])
    for cut in shards[1:]:
        factor_of = factor_of * one(*cut)
    return factor_of


def scatter_about(rng, extent, scale, most, cuts=(), kind=jnp.bfloat16):
    gain = shard_levels(rng, extent, cuts, -0.22, 0.18) if cuts else 1.0
    entries = jax.random.normal(rng, extent, jnp.float32) * scale * gain
    return jnp.minimum(jnp.maximum(entries, -most), most).astype(kind)


def setup_inputs(seed: int = 0) -> dict:
    streams_of = jax.random.split(jax.random.key(seed), 11)
    return {
        "starting_state": jnp.clip(jax.random.uniform(streams_of[0], (NODES, WIDTH), jnp.float32, -1.0, 1.0) * shard_levels(streams_of[0], (NODES, WIDTH), ((0, 512),), -0.4, 0.0), -1.0, 1.0),
        "features": scatter_about(streams_of[1], (NODES, INPUTS), 1.0, 6.0, ((0, 512),), jnp.float32),
        "cotangent": scatter_about(streams_of[2], (NODES, WIDTH), 1.0, 6.0, ((0, 512),), jnp.float32),
        "degrees": with_ends(jax.random.randint(streams_of[3], (NODES,), 8, 65), jax.random.fold_in(streams_of[3], 1), 8, 64).astype(jnp.int32),
        "tile_values": draw_tile_values(jax.random.fold_in(streams_of[10], 71), 0),
        "tile_rows": draw_tile_rows(jax.random.fold_in(streams_of[10], 71), 0),
        "tile_cols": draw_tile_cols(jax.random.fold_in(streams_of[10], 71), 0),
        "tile_live": draw_tile_live(jax.random.fold_in(streams_of[10], 71), 0),
        "weight": scatter_about(streams_of[8], (WIDTH, WIDTH), WIDTH ** -0.5, 0.375, (), jnp.float32),
        "input_map": scatter_about(streams_of[9], (INPUTS, WIDTH), INPUTS ** -0.5, 0.5, (), jnp.float32),
    }


PRECISION_HIGH = lax.Precision.HIGHEST

def forward_partial(values, rows_here, cols_here, live_here, row_block):
    blocks = row_block.reshape(TILE_ROWS, BLOCK, WIDTH)
    picked = jnp.take(blocks, rows_here, axis=0).astype(jnp.float32)
    matrix_products = jnp.einsum('tab,taf->tbf', values.astype(jnp.float32), picked, precision=PRECISION_HIGH)
    columns = jnp.arange(TILE_COLS).astype(jnp.int32)
    tile_assignment = ((cols_here[:, None] == columns[None, :]) & (live_here[:, None] == 1)).astype(jnp.float32)
    partial_result_value = jnp.einsum('sl,sxm->lxm', tile_assignment, matrix_products, precision=PRECISION_HIGH)
    return partial_result_value.reshape(TILE_COLS * BLOCK, WIDTH).astype(jnp.bfloat16)

def adjoint_partial(values, rows_here, cols_here, live_here, col_block):
    blocks = col_block.reshape(TILE_COLS, BLOCK, WIDTH)
    picked = jnp.take(blocks, cols_here, axis=0).astype(jnp.float32)
    matrix_products = jnp.einsum('tab,tbf->taf', values.astype(jnp.float32), picked, precision=PRECISION_HIGH)
    sources = jnp.arange(TILE_ROWS).astype(jnp.int32)
    tile_assignment = ((rows_here[:, None] == sources[None, :]) & (live_here[:, None] == 1)).astype(jnp.float32)
    partial_result_value = jnp.einsum('tr,taf->raf', tile_assignment, matrix_products, precision=PRECISION_HIGH)
    return partial_result_value.reshape(TILE_ROWS * BLOCK, WIDTH).astype(jnp.bfloat16)

def forward_sum(scaled, tile_values, tile_rows, tile_cols, tile_live):
    layout = scaled.reshape(N_ROW, N_COL * NODE_DEV, WIDTH)

    def add_row(totals, row_index):

        def one_col(col_index):
            return forward_partial(tile_values[row_index, col_index], tile_rows[row_index, col_index], tile_cols[row_index, col_index], tile_live[row_index, col_index], layout[row_index])
        partials = lax.map(one_col, jnp.arange(N_COL).astype(jnp.int32))
        return (totals + partials.astype(jnp.float32), None)
    initial = jnp.zeros((N_COL, N_ROW * NODE_DEV, WIDTH), jnp.float32)
    totals, ignored = lax.scan(add_row, initial, jnp.arange(N_ROW).astype(jnp.int32))
    totals = totals.reshape(N_COL, N_ROW, NODE_DEV, WIDTH).transpose(1, 0, 2, 3)
    return totals.reshape(N_ROW * N_COL * NODE_DEV, WIDTH)

def adjoint_sum(scaled, tile_values, tile_rows, tile_cols, tile_live):
    layout = scaled.reshape(N_ROW, N_COL, NODE_DEV, WIDTH)

    def add_col(totals, col_index):
        col_block = lax.dynamic_index_in_dim(layout, col_index, 1, keepdims=False)
        col_block = col_block.reshape(N_ROW * NODE_DEV, WIDTH)

        def one_row(row_index):
            return adjoint_partial(tile_values[row_index, col_index], tile_rows[row_index, col_index], tile_cols[row_index, col_index], tile_live[row_index, col_index], col_block)
        partials = lax.map(one_row, jnp.arange(N_ROW).astype(jnp.int32))
        return (totals + partials.astype(jnp.float32), None)
    initial = jnp.zeros((N_ROW, N_COL * NODE_DEV, WIDTH), jnp.float32)
    totals, ignored = lax.scan(add_col, initial, jnp.arange(N_COL).astype(jnp.int32))
    return totals.reshape(N_ROW * N_COL * NODE_DEV, WIDTH)

def reference(starting_state, features, cotangent, degrees, tile_values, tile_rows, tile_cols, tile_live, weight, input_map):
    reciprocal_square_root = lax.rsqrt(degrees.astype(jnp.float32))[:, None]
    driving = jnp.dot(features, input_map, precision=PRECISION_HIGH)
    states = starting_state
    summed = starting_state
    for sweep in range(ITERS):
        scaled = (reciprocal_square_root * states).astype(jnp.bfloat16)
        summed = reciprocal_square_root * forward_sum(scaled, tile_values, tile_rows, tile_cols, tile_live)
        states = jnp.tanh(jnp.dot(summed, weight, precision=PRECISION_HIGH) + driving)
    slopes = 1.0 - states * states
    adjoint = cotangent
    for sweep in range(ITERS):
        scaled = (reciprocal_square_root * (slopes * adjoint)).astype(jnp.bfloat16)
        pulled = reciprocal_square_root * adjoint_sum(scaled, tile_values, tile_rows, tile_cols, tile_live)
        adjoint = cotangent + jnp.dot(pulled, weight.T, precision=PRECISION_HIGH)
    masked = slopes * adjoint
    factor = 1.0 / math.sqrt(NODES)
    weight_grad = jnp.dot(summed.T, masked, precision=PRECISION_HIGH) * factor
    input_grad = jnp.dot(features.T, masked, precision=PRECISION_HIGH) * factor
    return (states, adjoint, weight_grad, input_grad)
```

```python
import functools
import math

import jax
import jax.numpy as jnp
from jax import lax
from jax.experimental import pallas as pl
from jax.experimental.pallas import tpu as pltpu
from jax.sharding import Mesh, PartitionSpec as P

HIGH = lax.Precision.HIGHEST
BF16 = jnp.bfloat16
F32 = jnp.float32
CHIP = ("xl", "z")
COL = ("xh", "y")
ROW = ("xl", "z", "core")
UNROLL = 4
VMEM = pl.BlockSpec(memory_space=pltpu.VMEM)
SMEM = pl.BlockSpec(memory_space=pltpu.SMEM)
ANY = pl.BlockSpec(memory_space=pl.ANY)


def shape(dims, dtype):
    return jax.ShapeDtypeStruct(dims, dtype)


def first_kernel(state, inv_col, out):
    scaled = jnp.transpose(state[...] * inv_col[...]).astype(BF16)
    for q in range(out.shape[0]):
        out[q] = scaled


def live_count(live):
    return lax.fori_loop(0, live.shape[0], lambda t, n: n + live[t], jnp.int32(0))


def place(c, core, half):
    return ((c & 1) ^ core) * half + (c >> 1)


def forward_kernel(rows, cols, live, core_ref, values, blocks, keep, send, acc):
    core = core_ref[0]
    half = keep.shape[0]
    acc[...] = jnp.zeros_like(acc)

    def group(g, carry):
        products, slots = [], []
        for u in range(UNROLL):
            t = g * UNROLL + u
            slot = place(cols[t], core, half)
            slots.append(jnp.where(live[t] == 1, slot, 2 * half))
            products.append(
                jnp.dot(blocks[rows[t]], values[t], preferred_element_type=F32)
            )
        for slot, product in zip(slots, products):
            acc[slot] += product
        return carry

    lax.fori_loop(0, (live_count(live) + UNROLL - 1) // UNROLL, group, 0)
    keep[...] = acc[0:half].astype(BF16)
    send[...] = acc[half : 2 * half].astype(BF16)


def adjoint_kernel(rows, cols, live, core_ref, values, own, other, out, blocks, acc, sem):
    core = core_ref[0]
    half = own.shape[0]
    count = out.shape[0]
    copies = [
        pltpu.make_async_copy(own, blocks.at[pl.ds(0, half)], sem.at[0]),
        pltpu.make_async_copy(other, blocks.at[pl.ds(half, half)], sem.at[1]),
    ]
    for copy in copies:
        copy.start()
    acc[...] = jnp.zeros_like(acc)
    groups = (live_count(live) + UNROLL - 1) // UNROLL
    for copy in copies:
        copy.wait()

    def group(g, carry):
        products, slots = [], []
        for u in range(UNROLL):
            t = g * UNROLL + u
            slots.append(jnp.where(live[t] == 1, rows[t], count))
            block = blocks[place(cols[t], core, half)]
            products.append(jnp.dot(values[t], block, preferred_element_type=F32))
        for slot, product in zip(slots, products):
            acc[slot] += product
        return carry

    lax.fori_loop(0, groups, group, 0)
    out[...] = acc[0:count].astype(BF16)


def state_kernel(parts, inv_row, inv_col, weight, features, input_map, cotangent, states, summed_t, out):
    total = parts[0].astype(F32)
    for q in range(1, parts.shape[0]):
        total += parts[q].astype(F32)
    total = total * inv_row[...]
    summed_t[...] = total
    driving = jnp.dot(features[...], input_map[...], precision=HIGH, preferred_element_type=F32)
    moved = lax.dot_general(
        jnp.transpose(total), weight[...], (((1,), (0,)), ((), ())), precision=HIGH, preferred_element_type=F32
    )
    state = jnp.tanh(moved + driving)
    states[...] = state
    slopes = 1.0 - state * state
    scaled = (inv_col[...] * (slopes * cotangent[...])).astype(BF16)
    for q in range(out.shape[0]):
        out[q] = scaled


def grad_kernel(core_ref, parts, inv_col, cotangent, weight, states, summed_t, features, adjoint, keep, send, *, factor):
    total = parts[0].astype(F32)
    for q in range(1, parts.shape[0]):
        total += parts[q].astype(F32)
    pulled = total * inv_col[...]
    moved = lax.dot_general(
        pulled, weight[...], (((1,), (1,)), ((), ())), precision=HIGH, preferred_element_type=F32
    )
    result = cotangent[...] + moved
    adjoint[...] = result
    state = states[...]
    masked = (1.0 - state * state) * result * factor
    weight_part = jnp.dot(summed_t[...], masked, precision=HIGH, preferred_element_type=F32)
    input_part = jnp.dot(
        jnp.transpose(features[...]), masked, precision=HIGH, preferred_element_type=F32
    )
    first = core_ref[0] == 0
    width = weight_part.shape[0]
    half = weight_part.shape[1] // 2
    for at, part in ((0, weight_part), (width, input_part)):
        left, right = part[:, :half], part[:, half:]
        keep[at : at + part.shape[0], :] = jnp.where(first, left, right)
        send[at : at + part.shape[0], :] = jnp.where(first, right, left)


def sum_kernel(parts, out):
    total = parts[0].astype(F32)
    for q in range(1, parts.shape[0]):
        total += parts[q].astype(F32)
    total = total.astype(out.dtype)
    for q in range(out.shape[0]):
        out[q] = total


def last_kernel(core_ref, own, other, weight_grad, input_grad):
    first = core_ref[0] == 0
    width = weight_grad.shape[0]
    half = own.shape[1]
    for at, out in ((0, weight_grad), (width, input_grad)):
        mine = own[at : at + out.shape[0], :].astype(F32)
        theirs = other[at : at + out.shape[0], :].astype(F32)
        out[:, :half] = jnp.where(first, mine, theirs)
        out[:, half:] = jnp.where(first, theirs, mine)


def call(kernel, outs, specs, scratch=(), name=None):
    return pl.pallas_call(
        kernel,
        out_shape=outs,
        in_specs=specs,
        out_specs=jax.tree.map(lambda _: VMEM, outs),
        scratch_shapes=list(scratch),
        name=name,
    )


def swap(x):
    return lax.ppermute(x, "core", [(0, 1), (1, 0)])


def exchange(x, axes):
    return lax.all_to_all(x, axes, 0, 0, tiled=True)


def on_device(
    starting_state,
    features,
    cotangent,
    degrees,
    tile_values,
    tile_rows,
    tile_cols,
    tile_live,
    weight,
    input_map,
):
    values = tile_values[0, 0]
    rows, cols, live = tile_rows[0, 0], tile_cols[0, 0], tile_live[0, 0]
    nodes, width = starting_state.shape
    inputs = features.shape[1]
    chips = lax.axis_size("xl") * lax.axis_size("z")
    col_devices = lax.axis_size("xh") * lax.axis_size("y")
    core = lax.axis_index("core").astype(jnp.int32).reshape(1)
    inverse = lax.rsqrt(degrees.astype(F32))
    inv_row, inv_col = inverse.reshape(1, nodes), inverse.reshape(nodes, 1)
    block = values.shape[1]

    spread = call(
        first_kernel, shape((col_devices, width, nodes), BF16), [VMEM] * 2, name="first"
    )(starting_state, inv_col)
    gathered = exchange(spread, COL)
    keep, send = call(
        forward_kernel,
        (shape((chips, width, block), BF16),) * 2,
        [SMEM] * 4 + [VMEM] * 2,
        [pltpu.VMEM((2 * chips + 1, width, block), F32)],
        name="forward",
    )(rows, cols, live, core, values, gathered)
    parts = exchange((keep.astype(F32) + swap(send).astype(F32)).astype(BF16), CHIP)
    states, summed_t, spread = call(
        state_kernel,
        (shape((nodes, width), F32), shape((width, nodes), F32), shape((chips, nodes, width), BF16)),
        [VMEM] * 7,
        name="state",
    )(parts, inv_row, inv_col, weight, features, input_map, cotangent)
    own = exchange(spread, CHIP)
    other = swap(own)
    partial = call(
        adjoint_kernel,
        shape((col_devices, block, width), BF16),
        [SMEM] * 4 + [VMEM] + [ANY] * 2,
        [
            pltpu.VMEM((2 * chips, block, width), BF16),
            pltpu.VMEM((col_devices + 1, block, width), F32),
            pltpu.SemaphoreType.DMA((2,)),
        ],
        name="adjoint",
    )(rows, cols, live, core, values, own, other)
    parts = exchange(partial, COL)
    factor = 1.0 / math.sqrt(nodes * 2 * chips * col_devices)
    total = width + inputs
    adjoint, keep, send = call(
        functools.partial(grad_kernel, factor=factor),
        (shape((nodes, width), F32), shape((total, width // 2), F32), shape((total, width // 2), F32)),
        [SMEM] + [VMEM] * 7,
        name="grad",
    )(core, parts, inv_col, cotangent, weight, states, summed_t, features)
    piece = (total // chips, width // 2)
    halves = (keep + swap(send)).reshape(chips, *piece)
    parts = exchange(halves, CHIP)
    spread = call(sum_kernel, shape((col_devices, *piece), F32), [VMEM], name="sum_chip")(parts)
    parts = exchange(spread, COL)
    spread = call(sum_kernel, shape((chips, *piece), BF16), [VMEM], name="sum_col")(parts)
    own = exchange(spread, CHIP).reshape(total, width // 2)
    other = swap(own)
    weight_grad, input_grad = call(
        last_kernel,
        (shape((width, width), F32), shape((inputs, width), F32)),
        [SMEM] + [VMEM] * 2,
        name="last",
    )(core, own, other)
    return states, adjoint, weight_grad, input_grad


def solution(mesh):
    sizes = mesh.devices.shape
    fine = Mesh(
        mesh.devices.reshape(2, sizes[0] // 4, 2, 2, sizes[1] // 2),
        ("xl", "z", "core", "xh", "y"),
    )
    every = ROW + COL
    return jax.shard_map(
        on_device,
        mesh=fine,
        in_specs=(
            P(every, None),
            P(every, None),
            P(every, None),
            P(every),
            P(ROW, COL, None, None, None),
            P(ROW, COL, None),
            P(ROW, COL, None),
            P(ROW, COL, None),
            P(),
            P(),
        ),
        out_specs=(P(every, None), P(every, None), P(), P()),
        check_vma=False,
    )
```

```python
import functools
import math

import jax
import jax.numpy as jnp
from jax import lax
from jax.experimental import pallas as pl
from jax.experimental.pallas import tpu as pltpu
from jax.sharding import Mesh, PartitionSpec as P

HIGH = lax.Precision.HIGHEST
BF16 = jnp.bfloat16
F32 = jnp.float32
CHIP = ("xl", "z")
COL = ("xh", "y")
ROW = ("xl", "z", "core")
UNROLL = 4
CHUNKS = 1
VMEM = pl.BlockSpec(memory_space=pltpu.VMEM)
SMEM = pl.BlockSpec(memory_space=pltpu.SMEM)
ANY = pl.BlockSpec(memory_space=pl.ANY)


def shape(dims, dtype):
    return jax.ShapeDtypeStruct(dims, dtype)


def chunk_of(width, h):
    size = width // CHUNKS
    return slice(h * size, (h + 1) * size)


def first_kernel(state, degrees, *outs):
    inverse = lax.rsqrt(degrees[...].astype(F32))
    scaled = (jnp.transpose(state[...]) * inverse).astype(BF16)
    for h, out in enumerate(outs):
        piece = scaled[chunk_of(scaled.shape[0], h), :]
        for q in range(out.shape[0]):
            out[q] = piece


def summed_up(parts):
    total = parts[0].astype(F32)
    for q in range(1, parts.shape[0]):
        total += parts[q].astype(F32)
    return total


def live_count(live):
    return lax.fori_loop(0, live.shape[0], lambda t, n: n + live[t], jnp.int32(0))


def place(c, core, half):
    return ((c & 1) ^ core) * half + (c >> 1)


def forward_kernel(rows, cols, live, core_ref, values, blocks, keep, send, acc):
    core = core_ref[0]
    half = keep.shape[0]
    acc[...] = jnp.zeros_like(acc)

    def group(g, carry):
        products, slots = [], []
        for u in range(UNROLL):
            t = g * UNROLL + u
            slot = place(cols[t], core, half)
            slots.append(jnp.where(live[t] == 1, slot, 2 * half))
            products.append(
                jnp.dot(blocks[rows[t]], values[t], preferred_element_type=F32)
            )
        for slot, product in zip(slots, products):
            acc[slot] += product
        return carry

    lax.fori_loop(0, (live_count(live) + UNROLL - 1) // UNROLL, group, 0)
    keep[...] = acc[0:half].astype(BF16)
    send[...] = acc[half : 2 * half].astype(BF16)


def adjoint_kernel(rows, cols, live, core_ref, values, own, other, out, blocks, acc, sem):
    core = core_ref[0]
    half = own.shape[0]
    count = out.shape[0]
    copies = [
        pltpu.make_async_copy(own, blocks.at[pl.ds(0, half)], sem.at[0]),
        pltpu.make_async_copy(other, blocks.at[pl.ds(half, half)], sem.at[1]),
    ]
    for copy in copies:
        copy.start()
    acc[...] = jnp.zeros_like(acc)
    groups = (live_count(live) + UNROLL - 1) // UNROLL
    for copy in copies:
        copy.wait()

    def group(g, carry):
        products, slots = [], []
        for u in range(UNROLL):
            t = g * UNROLL + u
            slots.append(jnp.where(live[t] == 1, rows[t], count))
            block = blocks[place(cols[t], core, half)]
            products.append(jnp.dot(values[t], block, preferred_element_type=F32))
        for slot, product in zip(slots, products):
            acc[slot] += product
        return carry

    lax.fori_loop(0, groups, group, 0)
    out[...] = acc[0:count].astype(BF16)


def state_kernel(*refs):
    parts = refs[:CHUNKS]
    inv_row, inv_col, weight, features, input_map, cotangent, states, summed_t = refs[CHUNKS : CHUNKS + 8]
    outs = refs[CHUNKS + 8 :]
    total = jnp.concatenate([summed_up(p) for p in parts], axis=0) * inv_row[...]
    summed_t[...] = total
    driving = jnp.dot(features[...], input_map[...], precision=HIGH, preferred_element_type=F32)
    moved = lax.dot_general(
        jnp.transpose(total), weight[...], (((1,), (0,)), ((), ())), precision=HIGH, preferred_element_type=F32
    )
    state = jnp.tanh(moved + driving)
    states[...] = state
    slopes = 1.0 - state * state
    scaled = (inv_col[...] * (slopes * cotangent[...])).astype(BF16)
    for h, out in enumerate(outs):
        piece = scaled[:, chunk_of(scaled.shape[1], h)]
        for q in range(out.shape[0]):
            out[q] = piece


def grad_kernel(core_ref, *refs, factor):
    parts = refs[:CHUNKS]
    inv_col, cotangent, weight, states, summed_t, features, adjoint, keep, send = refs[CHUNKS:]
    total = jnp.concatenate([summed_up(p) for p in parts], axis=1)
    pulled = total * inv_col[...]
    moved = lax.dot_general(
        pulled, weight[...], (((1,), (1,)), ((), ())), precision=HIGH, preferred_element_type=F32
    )
    result = cotangent[...] + moved
    adjoint[...] = result
    state = states[...]
    masked = (1.0 - state * state) * result * factor
    weight_part = jnp.dot(summed_t[...], masked, precision=HIGH, preferred_element_type=F32)
    input_part = jnp.dot(
        jnp.transpose(features[...]), masked, precision=HIGH, preferred_element_type=F32
    )
    first = core_ref[0] == 0
    width = weight_part.shape[0]
    half = weight_part.shape[1] // 2
    for at, part in ((0, weight_part), (width, input_part)):
        left, right = part[:, :half], part[:, half:]
        keep[at : at + part.shape[0], :] = jnp.where(first, left, right).astype(keep.dtype)
        send[at : at + part.shape[0], :] = jnp.where(first, right, left).astype(send.dtype)


def sum_kernel(parts, out):
    total = summed_up(parts).astype(out.dtype)
    for q in range(out.shape[0]):
        out[q] = total


def last_kernel(core_ref, own, other, weight_grad, input_grad):
    first = core_ref[0] == 0
    width = weight_grad.shape[0]
    half = own.shape[1]
    for at, out in ((0, weight_grad), (width, input_grad)):
        mine = own[at : at + out.shape[0], :].astype(F32)
        theirs = other[at : at + out.shape[0], :].astype(F32)
        out[:, :half] = jnp.where(first, mine, theirs)
        out[:, half:] = jnp.where(first, theirs, mine)


def call(kernel, outs, specs, scratch=(), name=None, mib=12, flops=10**8):
    return pl.pallas_call(
        kernel,
        out_shape=outs,
        in_specs=specs,
        out_specs=jax.tree.map(lambda _: VMEM, outs),
        scratch_shapes=list(scratch),
        name=name,
        compiler_params=pltpu.CompilerParams(vmem_limit_bytes=mib * 2**20),
        cost_estimate=pl.CostEstimate(flops=flops, bytes_accessed=2**21, transcendentals=0),
    )


def swap(x):
    return lax.ppermute(x, "core", [(0, 1), (1, 0)])


def exchange(x, axes):
    return lax.all_to_all(x, axes, 0, 0, tiled=True)


def on_device(
    starting_state,
    features,
    cotangent,
    degrees,
    tile_values,
    tile_rows,
    tile_cols,
    tile_live,
    weight,
    input_map,
):
    values = tile_values[0, 0]
    rows, cols, live = tile_rows[0, 0], tile_cols[0, 0], tile_live[0, 0]
    nodes, width = starting_state.shape
    inputs = features.shape[1]
    chips = lax.axis_size("xl") * lax.axis_size("z")
    col_devices = lax.axis_size("xh") * lax.axis_size("y")
    core = lax.axis_index("core").astype(jnp.int32).reshape(1)
    inverse = lax.rsqrt(degrees.astype(F32))
    inv_row, inv_col = inverse.reshape(1, nodes), inverse.reshape(nodes, 1)
    block = values.shape[1]
    size = width // CHUNKS
    tile_flops = 2 * values.shape[0] * block * block * size

    spreads = call(
        first_kernel, (shape((col_devices, size, nodes), BF16),) * CHUNKS, [VMEM] * 2, name="first"
    )(starting_state, degrees.reshape(1, nodes))
    forward = call(
        forward_kernel,
        (shape((chips, size, block), BF16),) * 2,
        [SMEM] * 4 + [VMEM] * 2,
        [pltpu.VMEM((2 * chips + 1, size, block), F32)],
        name="forward",
        mib=20,
        flops=tile_flops,
    )
    gathered = [exchange(spread, COL) for spread in spreads]
    parts = []
    for x in gathered:
        keep, send = forward(rows, cols, live, core, values, x)
        parts.append(exchange((keep.astype(F32) + swap(send).astype(F32)).astype(BF16), CHIP))
    states, summed_t, *spreads = call(
        state_kernel,
        (shape((nodes, width), F32), shape((width, nodes), F32))
        + (shape((chips, nodes, size), BF16),) * CHUNKS,
        [VMEM] * (CHUNKS + 6),
        name="state",
    )(*parts, inv_row, inv_col, weight, features, input_map, cotangent)
    adjoint_sum = call(
        adjoint_kernel,
        shape((col_devices, block, size), BF16),
        [SMEM] * 4 + [VMEM] + [ANY] * 2,
        [
            pltpu.VMEM((2 * chips, block, size), BF16),
            pltpu.VMEM((col_devices + 1, block, size), F32),
            pltpu.SemaphoreType.DMA((2,)),
        ],
        name="adjoint",
        mib=20,
        flops=tile_flops,
    )
    gathered = [exchange(spread, CHIP) for spread in spreads]
    parts = []
    for own in gathered:
        partial = adjoint_sum(rows, cols, live, core, values, own, swap(own))
        parts.append(exchange(partial, COL))
    factor = 1.0 / math.sqrt(nodes * 2 * chips * col_devices)
    total = width + inputs
    adjoint, keep, send = call(
        functools.partial(grad_kernel, factor=factor),
        (shape((nodes, width), F32),) + (shape((total, width // 2), BF16),) * 2,
        [SMEM] + [VMEM] * (CHUNKS + 6),
        name="grad",
    )(core, *parts, inv_col, cotangent, weight, states, summed_t, features)
    piece = (total // chips, width // 2)
    halves = (keep.astype(F32) + swap(send).astype(F32)).astype(BF16).reshape(chips, *piece)
    parts = exchange(halves, CHIP)
    spread = call(sum_kernel, shape((col_devices, *piece), BF16), [VMEM], name="sum_chip")(parts)
    parts = exchange(spread, COL)
    spread = call(sum_kernel, shape((chips, *piece), BF16), [VMEM], name="sum_col")(parts)
    own = exchange(spread, CHIP).reshape(total, width // 2)
    other = swap(own)
    weight_grad, input_grad = call(
        last_kernel,
        (shape((width, width), F32), shape((inputs, width), F32)),
        [SMEM] + [VMEM] * 2,
        name="last",
    )(core, own, other)
    return states, adjoint, weight_grad, input_grad


def solution(mesh):
    sizes = mesh.devices.shape
    fine = Mesh(
        mesh.devices.reshape(2, sizes[0] // 4, 2, 2, sizes[1] // 2),
        ("xl", "z", "core", "xh", "y"),
    )
    every = ROW + COL
    return jax.shard_map(
        on_device,
        mesh=fine,
        in_specs=(
            P(every, None),
            P(every, None),
            P(every, None),
            P(every),
            P(ROW, COL, None, None, None),
            P(ROW, COL, None),
            P(ROW, COL, None),
            P(ROW, COL, None),
            P(),
            P(),
        ),
        out_specs=(P(every, None), P(every, None), P(), P()),
        check_vma=False,
    )
```

```python
import functools
import math

import jax
import jax.numpy as jnp
from jax import lax
from jax.experimental import pallas as pl
from jax.experimental.pallas import tpu as pltpu
from jax.sharding import Mesh, PartitionSpec as P

HIGH = lax.Precision.HIGHEST
BF16 = jnp.bfloat16
F32 = jnp.float32
CHIP = ("xl", "z")
COL = ("xh", "y")
ROW = ("xl", "z", "core")
UNROLL = 4
FIRST_MIB = 56
VMEM = pl.BlockSpec(memory_space=pltpu.VMEM)
SMEM = pl.BlockSpec(memory_space=pltpu.SMEM)


def shape(dims, dtype):
    return jax.ShapeDtypeStruct(dims, dtype)


def summed_up(parts):
    total = parts[0].astype(F32)
    for q in range(1, parts.shape[0]):
        total += parts[q].astype(F32)
    return total


def first_kernel(state, degrees, out):
    inverse = lax.rsqrt(degrees[...].astype(F32))
    scaled = (jnp.transpose(state[...]) * inverse).astype(BF16)
    for q in range(out.shape[0]):
        out[q] = scaled


def prep_kernel(
    rows, cols, live, core_ref, degrees, features, input_map, cotangent,
    tiles, rows_of, cols_of, counts, inv_row, inv_wide, driving, features_t, cotangent_scaled,
):
    core = core_ref[0]
    slots = live.shape[0]

    def clear(t, carry):
        for side in range(2):
            tiles[side, t] = 0
            rows_of[side, t] = 0
            cols_of[side, t] = 0
        return carry

    lax.fori_loop(0, tiles.shape[1], clear, 0)

    def sort(t, ends):
        side = (cols[t] & 1) ^ core
        at = jnp.where(side == 0, ends[0], ends[1])
        use = live[t] == 1

        @pl.when(use)
        def _():
            tiles[side, at] = t
            rows_of[side, at] = rows[t]
            cols_of[side, at] = cols[t] >> 1

        one = use.astype(jnp.int32)
        return ends[0] + jnp.where(side == 0, one, 0), ends[1] + jnp.where(side == 1, one, 0)

    own, other = lax.fori_loop(0, slots, sort, (jnp.int32(0), jnp.int32(0)))
    counts[0] = own
    counts[1] = other
    inverse = lax.rsqrt(degrees[...].astype(F32))
    inv_row[...] = inverse
    wide = jnp.transpose(jnp.broadcast_to(inverse, inv_wide.shape))
    inv_wide[...] = wide
    features_t[...] = jnp.transpose(features[...])
    driving[...] = jnp.dot(
        features[...], input_map[...], precision=HIGH, preferred_element_type=F32
    )
    cotangent_scaled[...] = cotangent[...] * wide[:, :1]


def add_tiles(side, counts, tiles, slots_of, blocks_of, product_of, acc):
    count = counts[side]
    spare = acc.shape[0] - 1

    def group(g, carry):
        products, slots = [], []
        for u in range(UNROLL):
            t = g * UNROLL + u
            slots.append(jnp.where(t < count, slots_of[side, t], spare))
            products.append(product_of(tiles[side, t], blocks_of[side, t]))
        for slot, product in zip(slots, products):
            acc[slot] += product
        return carry

    lax.fori_loop(0, (count + UNROLL - 1) // UNROLL, group, 0)


def forward_kernel(counts, tiles, rows_of, cols_of, values, blocks, out, acc, *, side):
    acc[...] = jnp.zeros_like(acc)

    def product_of(tile, block):
        return jnp.dot(blocks[block], values[tile], preferred_element_type=F32)

    add_tiles(side, counts, tiles, cols_of, rows_of, product_of, acc)
    out[...] = acc[0 : out.shape[0]].astype(BF16)


def adjoint_own_kernel(counts, tiles, rows_of, cols_of, values, blocks, acc):
    acc[...] = jnp.zeros_like(acc)

    def product_of(tile, block):
        return jnp.dot(values[tile], blocks[block], preferred_element_type=F32)

    add_tiles(0, counts, tiles, rows_of, cols_of, product_of, acc)


def adjoint_other_kernel(counts, tiles, rows_of, cols_of, values, blocks, start, out, acc):
    acc[...] = start[...]

    def product_of(tile, block):
        return jnp.dot(values[tile], blocks[block], preferred_element_type=F32)

    add_tiles(1, counts, tiles, rows_of, cols_of, product_of, acc)
    out[...] = acc[0 : out.shape[0]].astype(BF16)


def state_kernel(parts, inv_row, weight, driving, cotangent_scaled, states, summed_t, out):
    total = summed_up(parts) * inv_row[...]
    summed_t[...] = total
    moved = jnp.dot(jnp.transpose(total), weight[...], precision=HIGH, preferred_element_type=F32)
    state = jnp.tanh(moved + driving[...])
    states[...] = state
    slopes = 1.0 - state * state
    scaled = (slopes * cotangent_scaled[...]).astype(BF16)
    for q in range(out.shape[0]):
        out[q] = scaled


def grad_kernel(
    core_ref, parts, inv_wide, cotangent, weight, states, summed_t, features_t, adjoint, keep, send, *, factor
):
    pulled = summed_up(parts) * inv_wide[:, :1]
    moved = lax.dot_general(
        pulled, weight[...], (((1,), (1,)), ((), ())), precision=HIGH, preferred_element_type=F32
    )
    result = cotangent[...] + moved
    adjoint[...] = result
    state = states[...]
    masked = (1.0 - state * state) * result * factor
    weight_part = jnp.dot(summed_t[...], masked, precision=HIGH, preferred_element_type=F32)
    input_part = jnp.dot(features_t[...], masked, precision=HIGH, preferred_element_type=F32)
    first = core_ref[0] == 0
    width = weight_part.shape[0]
    half = weight_part.shape[1] // 2
    for at, part in ((0, weight_part), (width, input_part)):
        left, right = part[:, :half], part[:, half:]
        keep[at : at + part.shape[0], :] = jnp.where(first, left, right).astype(keep.dtype)
        send[at : at + part.shape[0], :] = jnp.where(first, right, left).astype(send.dtype)


def sum_kernel(parts, out):
    total = summed_up(parts).astype(out.dtype)
    for q in range(out.shape[0]):
        out[q] = total


def last_kernel(core_ref, own, other, weight_grad, input_grad):
    first = core_ref[0] == 0
    width = weight_grad.shape[0]
    half = own.shape[1]
    for at, out in ((0, weight_grad), (width, input_grad)):
        mine = own[at : at + out.shape[0], :].astype(F32)
        theirs = other[at : at + out.shape[0], :].astype(F32)
        out[:, :half] = jnp.where(first, mine, theirs)
        out[:, half:] = jnp.where(first, theirs, mine)


def call(kernel, outs, specs, scratch=(), name=None, mib=12, flops=10**8, out_specs=None):
    return pl.pallas_call(
        kernel,
        out_shape=outs,
        in_specs=specs,
        out_specs=jax.tree.map(lambda _: VMEM, outs) if out_specs is None else out_specs,
        scratch_shapes=list(scratch),
        name=name,
        compiler_params=pltpu.CompilerParams(vmem_limit_bytes=mib * 2**20),
        cost_estimate=pl.CostEstimate(flops=flops, bytes_accessed=2**21, transcendentals=0),
    )


def swap(x):
    return lax.ppermute(x, "core", [(0, 1), (1, 0)])


def exchange(x, axes):
    return lax.all_to_all(x, axes, 0, 0, tiled=True)


def on_device(
    starting_state,
    features,
    cotangent,
    degrees,
    tile_values,
    tile_rows,
    tile_cols,
    tile_live,
    weight,
    input_map,
):
    values = tile_values[0, 0]
    rows, cols, live = tile_rows[0, 0], tile_cols[0, 0], tile_live[0, 0]
    nodes, width = starting_state.shape
    inputs = features.shape[1]
    chips = lax.axis_size("xl") * lax.axis_size("z")
    col_devices = lax.axis_size("xh") * lax.axis_size("y")
    core = lax.axis_index("core").astype(jnp.int32).reshape(1)
    degree_row = degrees.reshape(1, nodes)
    block = values.shape[1]
    room = values.shape[0] + UNROLL
    tile_flops = values.shape[0] * block * block * width

    spread = call(
        first_kernel, shape((col_devices, width, nodes), BF16), [VMEM] * 2, name="first", mib=FIRST_MIB
    )(starting_state, degree_row)
    gathered = exchange(spread, COL)
    lists = (shape((2, room), jnp.int32),) * 3 + (shape((2,), jnp.int32),)
    tiles, rows_of, cols_of, counts, inv_row, inv_wide, driving, features_t, cotangent_scaled = call(
        prep_kernel,
        lists
        + (
            shape((1, nodes), F32),
            shape((nodes, nodes), F32),
            shape((nodes, width), F32),
            shape((inputs, nodes), F32),
            shape((nodes, width), F32),
        ),
        [SMEM] * 4 + [VMEM] * 4,
        name="prep",
        out_specs=(SMEM,) * 4 + (VMEM,) * 5,
    )(rows, cols, live, core, degree_row, features, input_map, cotangent)
    order = (counts, tiles, rows_of, cols_of, values)

    def forward(side):
        return call(
            functools.partial(forward_kernel, side=side),
            shape((chips, width, block), BF16),
            [SMEM] * 4 + [VMEM] * 2,
            [pltpu.VMEM((chips + 1, width, block), F32)],
            name=f"forward{side}",
            flops=tile_flops,
        )(*order, gathered)

    received = swap(forward(1))
    parts = exchange((forward(0).astype(F32) + received.astype(F32)).astype(BF16), CHIP)
    states, summed_t, spread = call(
        state_kernel,
        (shape((nodes, width), F32), shape((width, nodes), F32), shape((chips, nodes, width), BF16)),
        [VMEM] * 5,
        name="state",
    )(parts, inv_row, weight, driving, cotangent_scaled)
    own = exchange(spread, CHIP)
    other = swap(own)
    total = (col_devices + 1, block, width)
    part_sum = call(
        adjoint_own_kernel,
        shape(total, F32),
        [SMEM] * 4 + [VMEM] * 2,
        name="adjoint0",
        flops=tile_flops,
    )(*order, own)
    partial = call(
        adjoint_other_kernel,
        shape((col_devices, block, width), BF16),
        [SMEM] * 4 + [VMEM] * 3,
        [pltpu.VMEM(total, F32)],
        name="adjoint1",
        flops=tile_flops,
    )(*order, other, part_sum)
    parts = exchange(partial, COL)
    factor = 1.0 / math.sqrt(nodes * 2 * chips * col_devices)
    total = width + inputs
    adjoint, keep, send = call(
        functools.partial(grad_kernel, factor=factor),
        (shape((nodes, width), F32),) + (shape((total, width // 2), BF16),) * 2,
        [SMEM] + [VMEM] * 7,
        name="grad",
    )(core, parts, inv_wide, cotangent, weight, states, summed_t, features_t)
    piece = (total // chips, width // 2)
    halves = (keep.astype(F32) + swap(send).astype(F32)).astype(BF16).reshape(chips, *piece)
    parts = exchange(halves, CHIP)
    spread = call(sum_kernel, shape((col_devices, *piece), BF16), [VMEM], name="sum_chip")(parts)
    parts = exchange(spread, COL)
    spread = call(sum_kernel, shape((chips, *piece), BF16), [VMEM], name="sum_col")(parts)
    own = exchange(spread, CHIP).reshape(total, width // 2)
    other = swap(own)
    weight_grad, input_grad = call(
        last_kernel,
        (shape((width, width), F32), shape((inputs, width), F32)),
        [SMEM] + [VMEM] * 2,
        name="last",
    )(core, own, other)
    return states, adjoint, weight_grad, input_grad


def solution(mesh):
    sizes = mesh.devices.shape
    fine = Mesh(
        mesh.devices.reshape(2, sizes[0] // 4, 2, 2, sizes[1] // 2),
        ("xl", "z", "core", "xh", "y"),
    )
    every = ROW + COL
    return jax.shard_map(
        on_device,
        mesh=fine,
        in_specs=(
            P(every, None),
            P(every, None),
            P(every, None),
            P(every),
            P(ROW, COL, None, None, None),
            P(ROW, COL, None),
            P(ROW, COL, None),
            P(ROW, COL, None),
            P(),
            P(),
        ),
        out_specs=(P(every, None), P(every, None), P(), P()),
        check_vma=False,
    )
```

```python
import functools
import math

import jax
import jax.numpy as jnp
from jax import lax
from jax.experimental import pallas as pl
from jax.experimental.pallas import tpu as pltpu
from jax.sharding import Mesh, PartitionSpec as P

HIGH = lax.Precision.HIGHEST
BF16 = jnp.bfloat16
F32 = jnp.float32
CHIP = ("xl", "z")
COL = ("xh", "y")
ROW = ("xl", "z", "core")
UNROLL = 16
REST = 4
FIRST_MIB = 56
VMEM = pl.BlockSpec(memory_space=pltpu.VMEM)
SMEM = pl.BlockSpec(memory_space=pltpu.SMEM)


def shape(dims, dtype):
    return jax.ShapeDtypeStruct(dims, dtype)


def summed_up(parts):
    total = parts[0].astype(F32)
    for q in range(1, parts.shape[0]):
        total += parts[q].astype(F32)
    return total


def first_kernel(state, degrees, out):
    inverse = lax.rsqrt(degrees[...].astype(F32))
    scaled = (jnp.transpose(state[...]) * inverse).astype(BF16)
    for q in range(out.shape[0]):
        out[q] = scaled


def prep_kernel(
    rows, cols, live, core_ref, degrees, features, input_map, cotangent,
    tiles, rows_of, cols_of, counts, inv_row, inv_wide, driving, features_t, cotangent_scaled,
):
    core = core_ref[0]
    slots = live.shape[0]

    def clear(t, carry):
        for side in range(2):
            tiles[side, t] = 0
            rows_of[side, t] = 0
            cols_of[side, t] = 0
        return carry

    lax.fori_loop(0, tiles.shape[1], clear, 0)

    def sort(t, ends):
        side = (cols[t] & 1) ^ core
        at = jnp.where(side == 0, ends[0], ends[1])
        use = live[t] == 1

        @pl.when(use)
        def _():
            tiles[side, at] = t
            rows_of[side, at] = rows[t]
            cols_of[side, at] = cols[t] >> 1

        one = use.astype(jnp.int32)
        return ends[0] + jnp.where(side == 0, one, 0), ends[1] + jnp.where(side == 1, one, 0)

    own, other = lax.fori_loop(0, slots, sort, (jnp.int32(0), jnp.int32(0)))
    counts[0] = own
    counts[1] = other
    inverse = lax.rsqrt(degrees[...].astype(F32))
    inv_row[...] = inverse
    wide = jnp.transpose(jnp.broadcast_to(inverse, inv_wide.shape))
    inv_wide[...] = wide
    features_t[...] = jnp.transpose(features[...])
    driving[...] = jnp.dot(
        features[...], input_map[...], precision=HIGH, preferred_element_type=F32
    )
    cotangent_scaled[...] = cotangent[...] * wide[:, :1]


def add_tiles(side, counts, tiles, slots_of, blocks_of, product_of, acc):
    count = counts[side]
    spare = acc.shape[0] - 1

    def group(size, start, g, carry):
        products, slots = [], []
        for u in range(size):
            t = start + g * size + u
            slots.append(jnp.where(t < count, slots_of[side, t], spare))
            products.append(product_of(tiles[side, t], blocks_of[side, t]))
        for slot, product in zip(slots, products):
            acc[slot] += product
        return carry

    full = count // UNROLL
    done = full * UNROLL
    lax.fori_loop(0, full, functools.partial(group, UNROLL, 0), 0)
    lax.fori_loop(0, (count - done + REST - 1) // REST, functools.partial(group, REST, done), 0)


def forward_own_kernel(counts, tiles, rows_of, cols_of, values, blocks, acc):
    acc[...] = jnp.zeros_like(acc)

    def product_of(tile, block):
        return jnp.dot(blocks[block], values[tile], preferred_element_type=F32)

    add_tiles(0, counts, tiles, cols_of, rows_of, product_of, acc)


def join_kernel(mine, received, out):
    for q in range(out.shape[0]):
        out[q] = (mine[q] + received[q].astype(F32)).astype(BF16)


def forward_other_kernel(counts, tiles, rows_of, cols_of, values, blocks, out, acc):
    acc[...] = jnp.zeros_like(acc)

    def product_of(tile, block):
        return jnp.dot(blocks[block], values[tile], preferred_element_type=F32)

    add_tiles(1, counts, tiles, cols_of, rows_of, product_of, acc)
    out[...] = acc[0 : out.shape[0]].astype(BF16)


def adjoint_own_kernel(counts, tiles, rows_of, cols_of, values, blocks, acc):
    acc[...] = jnp.zeros_like(acc)

    def product_of(tile, block):
        return jnp.dot(values[tile], blocks[block], preferred_element_type=F32)

    add_tiles(0, counts, tiles, rows_of, cols_of, product_of, acc)


def adjoint_other_kernel(counts, tiles, rows_of, cols_of, values, blocks, start, out, acc):
    acc[...] = start[...]

    def product_of(tile, block):
        return jnp.dot(values[tile], blocks[block], preferred_element_type=F32)

    add_tiles(1, counts, tiles, rows_of, cols_of, product_of, acc)
    out[...] = acc[0 : out.shape[0]].astype(BF16)


def state_kernel(parts, inv_row, weight, driving, cotangent_scaled, states, summed_t, out):
    total = summed_up(parts) * inv_row[...]
    summed_t[...] = total
    moved = jnp.dot(jnp.transpose(total), weight[...], precision=HIGH, preferred_element_type=F32)
    state = jnp.tanh(moved + driving[...])
    states[...] = state
    slopes = 1.0 - state * state
    scaled = (slopes * cotangent_scaled[...]).astype(BF16)
    for q in range(out.shape[0]):
        out[q] = scaled


def grad_kernel(
    parts, inv_wide, cotangent, weight, states, summed_t, features_t, adjoint, out, *, factor
):
    pulled = summed_up(parts) * inv_wide[:, :1]
    moved = lax.dot_general(
        pulled, weight[...], (((1,), (1,)), ((), ())), precision=HIGH, preferred_element_type=F32
    )
    result = cotangent[...] + moved
    adjoint[...] = result
    state = states[...]
    masked = (1.0 - state * state) * result * factor
    weight_part = jnp.dot(summed_t[...], masked, precision=HIGH, preferred_element_type=F32)
    input_part = jnp.dot(features_t[...], masked, precision=HIGH, preferred_element_type=F32)
    half = out.shape[1]
    at = 0
    for side in range(2):
        for part in (weight_part, input_part):
            piece = part[:, side * half : (side + 1) * half]
            out[at : at + piece.shape[0], :] = piece.astype(out.dtype)
            at += piece.shape[0]


def sum_kernel(parts, out):
    total = summed_up(parts).astype(out.dtype)
    for q in range(out.shape[0]):
        out[q] = total


def last_kernel(sums, weight_grad, input_grad):
    half = sums.shape[1]
    at = 0
    for side in range(2):
        for out in (weight_grad, input_grad):
            out[:, side * half : (side + 1) * half] = sums[at : at + out.shape[0], :].astype(F32)
            at += out.shape[0]


def call(kernel, outs, specs, scratch=(), name=None, mib=12, flops=10**8, out_specs=None):
    return pl.pallas_call(
        kernel,
        out_shape=outs,
        in_specs=specs,
        out_specs=jax.tree.map(lambda _: VMEM, outs) if out_specs is None else out_specs,
        scratch_shapes=list(scratch),
        name=name,
        compiler_params=pltpu.CompilerParams(vmem_limit_bytes=mib * 2**20),
        cost_estimate=pl.CostEstimate(flops=flops, bytes_accessed=2**21, transcendentals=0),
    )


def swap(x):
    return lax.ppermute(x, "core", [(0, 1), (1, 0)])


def exchange(x, axes):
    return lax.all_to_all(x, axes, 0, 0, tiled=True)


def on_device(
    starting_state,
    features,
    cotangent,
    degrees,
    tile_values,
    tile_rows,
    tile_cols,
    tile_live,
    weight,
    input_map,
):
    values = tile_values[0, 0]
    rows, cols, live = tile_rows[0, 0], tile_cols[0, 0], tile_live[0, 0]
    nodes, width = starting_state.shape
    inputs = features.shape[1]
    chips = lax.axis_size("xl") * lax.axis_size("z")
    col_devices = lax.axis_size("xh") * lax.axis_size("y")
    core = lax.axis_index("core").astype(jnp.int32).reshape(1)
    degree_row = degrees.reshape(1, nodes)
    block = values.shape[1]
    room = values.shape[0] + REST
    tile_flops = values.shape[0] * block * block * width

    spread = call(
        first_kernel, shape((col_devices, width, nodes), BF16), [VMEM] * 2, name="first", mib=FIRST_MIB
    )(starting_state, degree_row)
    gathered = exchange(spread, COL)
    lists = (shape((2, room), jnp.int32),) * 3 + (shape((2,), jnp.int32),)
    tiles, rows_of, cols_of, counts, inv_row, inv_wide, driving, features_t, cotangent_scaled = call(
        prep_kernel,
        lists
        + (
            shape((1, nodes), F32),
            shape((nodes, nodes), F32),
            shape((nodes, width), F32),
            shape((inputs, nodes), F32),
            shape((nodes, width), F32),
        ),
        [SMEM] * 4 + [VMEM] * 4,
        name="prep",
        out_specs=(SMEM,) * 4 + (VMEM,) * 5,
    )(rows, cols, live, core, degree_row, features, input_map, cotangent)
    order = (counts, tiles, rows_of, cols_of, values)

    sent = call(
        forward_other_kernel,
        shape((chips, width, block), BF16),
        [SMEM] * 4 + [VMEM] * 2,
        [pltpu.VMEM((chips + 1, width, block), F32)],
        name="forward1",
        flops=tile_flops,
    )(*order, gathered)
    received = swap(sent)
    mine = call(
        forward_own_kernel,
        shape((chips + 1, width, block), F32),
        [SMEM] * 4 + [VMEM] * 2,
        name="forward0",
        flops=tile_flops,
    )(*order, gathered)
    joined = call(join_kernel, shape((chips, width, block), BF16), [VMEM] * 2, name="join")(
        mine, received
    )
    parts = exchange(joined, CHIP)
    states, summed_t, spread = call(
        state_kernel,
        (shape((nodes, width), F32), shape((width, nodes), F32), shape((chips, nodes, width), BF16)),
        [VMEM] * 5,
        name="state",
    )(parts, inv_row, weight, driving, cotangent_scaled)
    own = exchange(spread, CHIP)
    other = swap(own)
    total = (col_devices + 1, block, width)
    part_sum = call(
        adjoint_own_kernel,
        shape(total, F32),
        [SMEM] * 4 + [VMEM] * 2,
        name="adjoint0",
        flops=tile_flops,
    )(*order, own)
    partial = call(
        adjoint_other_kernel,
        shape((col_devices, block, width), BF16),
        [SMEM] * 4 + [VMEM] * 3,
        [pltpu.VMEM(total, F32)],
        name="adjoint1",
        flops=tile_flops,
    )(*order, other, part_sum)
    parts = exchange(partial, COL)
    factor = 1.0 / math.sqrt(nodes * 2 * chips * col_devices)
    total = width + inputs
    members = 2 * chips
    adjoint, sums = call(
        functools.partial(grad_kernel, factor=factor),
        (shape((nodes, width), F32), shape((2 * total, width // 2), BF16)),
        [VMEM] * 7,
        name="grad",
    )(parts, inv_wide, cotangent, weight, states, summed_t, features_t)
    piece = (2 * total // members, width // 2)
    parts = exchange(sums.reshape(members, *piece), ROW)
    spread = call(sum_kernel, shape((col_devices, *piece), BF16), [VMEM], name="sum_row")(parts)
    parts = exchange(spread, COL)
    spread = call(sum_kernel, shape((members, *piece), BF16), [VMEM], name="sum_col")(parts)
    sums = exchange(spread, ROW).reshape(2 * total, width // 2)
    weight_grad, input_grad = call(
        last_kernel,
        (shape((width, width), F32), shape((inputs, width), F32)),
        [VMEM],
        name="last",
    )(sums)
    return states, adjoint, weight_grad, input_grad


def solution(mesh):
    sizes = mesh.devices.shape
    fine = Mesh(
        mesh.devices.reshape(2, sizes[0] // 4, 2, 2, sizes[1] // 2),
        ("xl", "z", "core", "xh", "y"),
    )
    every = ROW + COL
    return jax.shard_map(
        on_device,
        mesh=fine,
        in_specs=(
            P(every, None),
            P(every, None),
            P(every, None),
            P(every),
            P(ROW, COL, None, None, None),
            P(ROW, COL, None),
            P(ROW, COL, None),
            P(ROW, COL, None),
            P(),
            P(),
        ),
        out_specs=(P(every, None), P(every, None), P(), P()),
        check_vma=False,
    )
```

```python
import functools
import math

import jax
import jax.numpy as jnp
from jax import lax
from jax.experimental import pallas as pl
from jax.experimental.pallas import tpu as pltpu
from jax.sharding import Mesh, PartitionSpec as P


HIGH = lax.Precision.HIGHEST
BF16 = jnp.bfloat16
F32 = jnp.float32
COL = ("xh", "y")
SIDE = ("core", "xh", "y")
ROW = ("xl", "z", "core")
UNROLL = 16
REST = 4
FIRST_MIB = 56
VMEM = pl.BlockSpec(memory_space=pltpu.VMEM)
ANY = pl.BlockSpec(memory_space=pl.ANY)
SMEM = pl.BlockSpec(memory_space=pltpu.SMEM)


def shape(dims, dtype):
    return jax.ShapeDtypeStruct(dims, dtype)


def summed_up(parts, first=0, step=1):
    total = parts[first].astype(F32)
    for q in range(first + step, parts.shape[0], step):
        total += parts[q].astype(F32)
    return total


def first_kernel(state, degrees, out):
    inverse = lax.rsqrt(degrees[...].astype(F32))
    scaled = (jnp.transpose(state[...]) * inverse).astype(BF16)
    half = out.shape[0] // 2
    size = out.shape[1]
    for q in range(half):
        out[q] = scaled[:size, :]
        out[half + q] = scaled[size:, :]


def pack_kernel(rows, cols, live, out):
    for q, x in enumerate((rows, cols, live)):
        out[q : q + 1, :] = x[...]


def prep_kernel(shared, values, degrees, features, input_map, cotangent, inv_row, inv_wide, driving, features_t, cotangent_scaled):
    inverse = lax.rsqrt(degrees[...].astype(F32))
    inv_row[...] = inverse
    wide = jnp.transpose(jnp.broadcast_to(inverse, inv_wide.shape))
    inv_wide[...] = wide
    features_t[...] = jnp.transpose(features[...])
    driving[...] = jnp.dot(
        features[...], input_map[...], precision=HIGH, preferred_element_type=F32
    )
    cotangent_scaled[...] = cotangent[...] * wide[:, :1]


def live_count(places):
    return lax.fori_loop(0, places.shape[1], lambda t, n: n + places[2, t], jnp.int32(0))


def add_tiles(places, core, values, forward, blocks, acc):
    count = live_count(places)
    spare = acc.shape[0] - 1
    start = core * (spare // 2 if not forward else blocks.shape[0] // 2)

    def group(size, begin, g, carry):
        products, slots = [], []
        for u in range(size):
            t = begin + g * size + u
            row, col = start + places[0, t], places[1, t]
            if forward:
                product = jnp.dot(blocks[row], values[t], preferred_element_type=F32)
            else:
                product = jnp.dot(values[t], blocks[col], preferred_element_type=F32)
            products.append(product)
            slots.append(jnp.where(t < count, col if forward else row, spare))
        for slot, product in zip(slots, products):
            acc[slot] += product
        return carry

    full = count // UNROLL
    done = full * UNROLL
    lax.fori_loop(0, full, functools.partial(group, UNROLL, 0), 0)
    lax.fori_loop(0, (count - done + REST - 1) // REST, functools.partial(group, REST, done), 0)


def tiles_kernel(core_ref, places, other_places, values, other_values, blocks, out, acc, held, sem, *, forward):
    core = core_ref[0]
    copy = pltpu.make_async_copy(other_values, held, sem)
    copy.start()
    acc[...] = jnp.zeros_like(acc)
    add_tiles(places, core, values, forward, blocks, acc)
    copy.wait()
    add_tiles(other_places, 1 - core, held, forward, blocks, acc)
    out[...] = acc[0 : out.shape[0]].astype(BF16)


def state_kernel(parts, inv_row, weight, driving, cotangent_scaled, states, summed_t, out):
    total = jnp.concatenate([summed_up(parts, 0, 2), summed_up(parts, 1, 2)], axis=0)
    total = total * inv_row[...]
    summed_t[...] = total
    moved = jnp.dot(jnp.transpose(total), weight[...], precision=HIGH, preferred_element_type=F32)
    state = jnp.tanh(moved + driving[...])
    states[...] = state
    slopes = 1.0 - state * state
    scaled = (slopes * cotangent_scaled[...]).astype(BF16)
    size = out.shape[2]
    for q in range(out.shape[0]):
        out[q] = scaled[:, (q % 2) * size : (q % 2 + 1) * size]


def grad_kernel(
    parts, inv_wide, cotangent, weight, states, summed_t, features_t, adjoint, out, *, factor
):
    middle = parts.shape[0] // 2
    total = jnp.concatenate(
        [summed_up(parts.at[pl.ds(0, middle)]), summed_up(parts.at[pl.ds(middle, middle)])], axis=1
    )
    pulled = total * inv_wide[:, :1]
    moved = lax.dot_general(
        pulled, weight[...], (((1,), (1,)), ((), ())), precision=HIGH, preferred_element_type=F32
    )
    result = cotangent[...] + moved
    adjoint[...] = result
    state = states[...]
    masked = (1.0 - state * state) * result * factor
    weight_part = jnp.dot(summed_t[...], masked, precision=HIGH, preferred_element_type=F32)
    input_part = jnp.dot(features_t[...], masked, precision=HIGH, preferred_element_type=F32)
    half = out.shape[1]
    at = 0
    for side in range(2):
        for part in (weight_part, input_part):
            piece = part[:, side * half : (side + 1) * half]
            out[at : at + piece.shape[0], :] = piece.astype(out.dtype)
            at += piece.shape[0]


def sum_kernel(parts, out):
    total = summed_up(parts).astype(out.dtype)
    for q in range(out.shape[0]):
        out[q] = total


def last_kernel(sums, weight_grad, input_grad):
    half = sums.shape[1]
    at = 0
    for side in range(2):
        for out in (weight_grad, input_grad):
            out[:, side * half : (side + 1) * half] = sums[at : at + out.shape[0], :].astype(F32)
            at += out.shape[0]


def call(kernel, outs, specs, scratch=(), mib=12, flops=10**8, out_specs=None):
    return pl.pallas_call(
        kernel,
        out_shape=outs,
        in_specs=specs,
        out_specs=jax.tree.map(lambda _: VMEM, outs) if out_specs is None else out_specs,
        scratch_shapes=list(scratch),
        compiler_params=pltpu.CompilerParams(vmem_limit_bytes=mib * 2**20),
        cost_estimate=pl.CostEstimate(flops=flops, bytes_accessed=2**21, transcendentals=0),
    )


def swap(x):
    return lax.ppermute(x, "core", [(0, 1), (1, 0)])


def exchange(x, axes):
    return lax.all_to_all(x, axes, 0, 0, tiled=True)


def body(
    starting_state,
    features,
    cotangent,
    degrees,
    tile_values,
    tile_rows,
    tile_cols,
    tile_live,
    weight,
    input_map,
):
    values = tile_values[0, 0]
    nodes, width = starting_state.shape
    inputs = features.shape[1]
    members = lax.axis_size(ROW)
    col_devices = lax.axis_size(COL)
    sides = 2 * col_devices
    core = lax.axis_index("core").astype(jnp.int32).reshape(1)
    degree_row = degrees.reshape(1, nodes)
    block = values.shape[1]
    size = width // 2
    places = call(
        pack_kernel, shape((3, values.shape[0]), jnp.int32), [VMEM] * 3, mib=4
    )(tile_rows[0], tile_cols[0], tile_live[0])

    spread = call(
        first_kernel, shape((sides, size, nodes), BF16), [VMEM] * 2, mib=FIRST_MIB
    )(starting_state, degree_row)
    gathered = exchange(spread, SIDE)
    other_places, other_values = swap(places), swap(values)
    prep = call(
        prep_kernel,
        (
            shape((1, nodes), F32),
            shape((nodes, nodes), F32),
            shape((nodes, width), F32),
            shape((inputs, nodes), F32),
            shape((nodes, width), F32),
        ),
        [ANY] + [VMEM] * 5,
    )
    inv_row, inv_wide, driving, features_t, cotangent_scaled = prep(
        other_values, values, degree_row, features, input_map, cotangent
    )
    order = (core, places, other_places, values, other_values)

    def tile_sums(forward, blocks, count, dims):
        return call(
            functools.partial(tiles_kernel, forward=forward),
            shape((count, *dims), BF16),
            [SMEM] * 3 + [VMEM, ANY, VMEM],
            [
                pltpu.VMEM((count + 1, *dims), F32),
                pltpu.VMEM(values.shape, BF16),
                pltpu.SemaphoreType.DMA,
            ],
            mib=16,
            flops=4 * values.shape[0] * block * block * size,
        )(*order, blocks)

    parts = exchange(tile_sums(True, gathered, members, (size, block)), ROW)
    states, summed_t, spread = call(
        state_kernel,
        (shape((nodes, width), F32), shape((width, nodes), F32), shape((members, nodes, size), BF16)),
        [VMEM] * 5,
    )(parts, inv_row, weight, driving, cotangent_scaled)
    blocks = exchange(spread, ROW)
    parts = exchange(tile_sums(False, blocks, sides, (block, size)), SIDE)
    factor = 1.0 / math.sqrt(nodes * members * col_devices)
    total = width + inputs
    adjoint, sums = call(
        functools.partial(grad_kernel, factor=factor),
        (shape((nodes, width), F32), shape((2 * total, width // 2), BF16)),
        [VMEM] * 7,
    )(parts, inv_wide, cotangent, weight, states, summed_t, features_t)
    piece = (2 * total // members, width // 2)
    parts = exchange(sums.reshape(members, *piece), ROW)
    spread = call(sum_kernel, shape((col_devices, *piece), BF16), [VMEM])(parts)
    parts = exchange(spread, COL)
    spread = call(sum_kernel, shape((members, *piece), BF16), [VMEM])(parts)
    sums = exchange(spread, ROW).reshape(2 * total, width // 2)
    weight_grad, input_grad = call(
        last_kernel, (shape((width, width), F32), shape((inputs, width), F32)), [VMEM]
    )(sums)
    return states, adjoint, weight_grad, input_grad


def solution(mesh):
    sizes = mesh.devices.shape
    fine = Mesh(
        mesh.devices.reshape(2, sizes[0] // 4, 2, 2, sizes[1] // 2),
        ("xl", "z", "core", "xh", "y"),
    )
    every = ROW + COL
    return jax.shard_map(
        body,
        mesh=fine,
        in_specs=(
            P(every, None),
            P(every, None),
            P(every, None),
            P(every),
            P(ROW, COL, None, None, None),
            P(ROW, COL, None),
            P(ROW, COL, None),
            P(ROW, COL, None),
            P(),
            P(),
        ),
        out_specs=(P(every, None), P(every, None), P(), P()),
        check_vma=False,
    )
```

```python
import functools
import math

import jax
import jax.numpy as jnp
from jax import lax
from jax.experimental import pallas as pl
from jax.experimental.pallas import tpu as pltpu
from jax.sharding import Mesh, PartitionSpec as P


HIGH = lax.Precision.HIGHEST
BF16 = jnp.bfloat16
F32 = jnp.float32
COL = ("xh", "y")
SIDE = ("core", "xh", "y")
ROW = ("xl", "z", "core")
UNROLL = 32
REST = 16
FIRST_MIB = 56
VMEM = pl.BlockSpec(memory_space=pltpu.VMEM)
ANY = pl.BlockSpec(memory_space=pl.ANY)
SMEM = pl.BlockSpec(memory_space=pltpu.SMEM)


def shape(dims, dtype):
    return jax.ShapeDtypeStruct(dims, dtype)


def summed_up(parts, first=0, step=1):
    total = parts[first].astype(F32)
    for q in range(first + step, parts.shape[0], step):
        total += parts[q].astype(F32)
    return total


def first_kernel(state, degrees, out):
    inverse = lax.rsqrt(degrees[...].astype(F32))
    scaled = (jnp.transpose(state[...]) * inverse).astype(BF16)
    half = out.shape[0] // 2
    size = out.shape[1]
    for q in range(half):
        out[q] = scaled[:size, :]
        out[half + q] = scaled[size:, :]


def pack_kernel(rows, cols, live, out):
    for q, x in enumerate((rows, cols)):
        out[q : q + 1, :] = x[...]
    count = jnp.sum(live[...].astype(F32), axis=1, keepdims=True)
    out[2:3, :] = jnp.broadcast_to(count, live.shape).astype(jnp.int32)


def prep_kernel(shared, values, degrees, features, input_map, cotangent, inv_row, inv_wide, driving, features_t, cotangent_scaled):
    inverse = lax.rsqrt(degrees[...].astype(F32))
    inv_row[...] = inverse
    wide = jnp.transpose(jnp.broadcast_to(inverse, inv_wide.shape))
    inv_wide[...] = wide
    features_t[...] = jnp.transpose(features[...])
    driving[...] = jnp.dot(
        features[...], input_map[...], precision=HIGH, preferred_element_type=F32
    )
    cotangent_scaled[...] = cotangent[...] * wide[:, :1]


def add_tiles(places, core, values, forward, blocks, acc):
    count = places[2, 0]
    spare = acc.shape[0] - 1
    start = core * (spare // 2 if not forward else blocks.shape[0] // 2)

    def group(size, begin, g, carry):
        products, slots = [], []
        for u in range(size):
            t = begin + g * size + u
            row, col = start + places[0, t], places[1, t]
            if forward:
                product = jnp.dot(blocks[row], values[t], preferred_element_type=F32)
            else:
                product = jnp.dot(values[t], blocks[col], preferred_element_type=F32)
            products.append(product)
            slots.append(jnp.where(t < count, col if forward else row, spare))
        for slot, product in zip(slots, products):
            acc[slot] += product
        return carry

    full = count // UNROLL
    done = full * UNROLL
    lax.fori_loop(0, full, functools.partial(group, UNROLL, 0), 0)
    lax.fori_loop(0, (count - done + REST - 1) // REST, functools.partial(group, REST, done), 0)


def tiles_kernel(core_ref, places, other_places, values, other_values, blocks, out, acc, held, sem, *, forward):
    core = core_ref[0]
    copy = pltpu.make_async_copy(other_values, held, sem)
    copy.start()
    acc[...] = jnp.zeros_like(acc)
    add_tiles(places, core, values, forward, blocks, acc)
    copy.wait()
    add_tiles(other_places, 1 - core, held, forward, blocks, acc)
    out[...] = acc[0 : out.shape[0]].astype(BF16)


def state_kernel(parts, inv_row, weight, driving, cotangent_scaled, states, summed_t, out):
    total = jnp.concatenate([summed_up(parts, 0, 2), summed_up(parts, 1, 2)], axis=0)
    total = total * inv_row[...]
    summed_t[...] = total
    moved = jnp.dot(jnp.transpose(total), weight[...], precision=HIGH, preferred_element_type=F32)
    state = jnp.tanh(moved + driving[...])
    states[...] = state
    slopes = 1.0 - state * state
    scaled = (slopes * cotangent_scaled[...]).astype(BF16)
    size = out.shape[2]
    for q in range(out.shape[0]):
        out[q] = scaled[:, (q % 2) * size : (q % 2 + 1) * size]


def grad_kernel(
    parts, inv_wide, cotangent, weight, states, summed_t, features_t, adjoint, out, *, factor
):
    middle = parts.shape[0] // 2
    total = jnp.concatenate(
        [summed_up(parts.at[pl.ds(0, middle)]), summed_up(parts.at[pl.ds(middle, middle)])], axis=1
    )
    pulled = total * inv_wide[:, :1]
    moved = lax.dot_general(
        pulled, weight[...], (((1,), (1,)), ((), ())), precision=HIGH, preferred_element_type=F32
    )
    result = cotangent[...] + moved
    adjoint[...] = result
    state = states[...]
    masked = (1.0 - state * state) * result * factor
    weight_part = jnp.dot(summed_t[...], masked, precision=HIGH, preferred_element_type=F32)
    input_part = jnp.dot(features_t[...], masked, precision=HIGH, preferred_element_type=F32)
    half = out.shape[1]
    at = 0
    for side in range(2):
        for part in (weight_part, input_part):
            piece = part[:, side * half : (side + 1) * half]
            out[at : at + piece.shape[0], :] = piece.astype(out.dtype)
            at += piece.shape[0]


def sum_kernel(parts, out):
    total = summed_up(parts).astype(out.dtype)
    for q in range(out.shape[0]):
        out[q] = total


def last_kernel(sums, weight_grad, input_grad):
    half = sums.shape[1]
    at = 0
    for side in range(2):
        for out in (weight_grad, input_grad):
            out[:, side * half : (side + 1) * half] = sums[at : at + out.shape[0], :].astype(F32)
            at += out.shape[0]


def call(kernel, outs, specs, scratch=(), mib=12, flops=10**8, out_specs=None):
    return pl.pallas_call(
        kernel,
        out_shape=outs,
        in_specs=specs,
        out_specs=jax.tree.map(lambda _: VMEM, outs) if out_specs is None else out_specs,
        scratch_shapes=list(scratch),
        compiler_params=pltpu.CompilerParams(vmem_limit_bytes=mib * 2**20),
        cost_estimate=pl.CostEstimate(flops=flops, bytes_accessed=2**21, transcendentals=0),
    )


def swap(x):
    return lax.ppermute(x, "core", [(0, 1), (1, 0)])


def exchange(x, axes):
    return lax.all_to_all(x, axes, 0, 0, tiled=True)


def body(
    starting_state,
    features,
    cotangent,
    degrees,
    tile_values,
    tile_rows,
    tile_cols,
    tile_live,
    weight,
    input_map,
):
    values = tile_values[0, 0]
    nodes, width = starting_state.shape
    inputs = features.shape[1]
    members = lax.axis_size(ROW)
    col_devices = lax.axis_size(COL)
    sides = 2 * col_devices
    core = lax.axis_index("core").astype(jnp.int32).reshape(1)
    degree_row = degrees.reshape(1, nodes)
    block = values.shape[1]
    size = width // 2
    places = call(
        pack_kernel, shape((3, values.shape[0]), jnp.int32), [VMEM] * 3, mib=4
    )(tile_rows[0], tile_cols[0], tile_live[0])

    spread = call(
        first_kernel, shape((sides, size, nodes), BF16), [VMEM] * 2, mib=FIRST_MIB
    )(starting_state, degree_row)
    gathered = exchange(spread, SIDE)
    other_places, other_values = swap(places), swap(values)
    prep = call(
        prep_kernel,
        (
            shape((1, nodes), F32),
            shape((nodes, nodes), F32),
            shape((nodes, width), F32),
            shape((inputs, nodes), F32),
            shape((nodes, width), F32),
        ),
        [ANY] + [VMEM] * 5,
    )
    inv_row, inv_wide, driving, features_t, cotangent_scaled = prep(
        other_values, values, degree_row, features, input_map, cotangent
    )
    order = (core, places, other_places, values, other_values)

    def tile_sums(forward, blocks, count, dims):
        return call(
            functools.partial(tiles_kernel, forward=forward),
            shape((count, *dims), BF16),
            [SMEM] * 3 + [VMEM, ANY, VMEM],
            [
                pltpu.VMEM((count + 1, *dims), F32),
                pltpu.VMEM(values.shape, BF16),
                pltpu.SemaphoreType.DMA,
            ],
            mib=16,
            flops=4 * values.shape[0] * block * block * size,
        )(*order, blocks)

    parts = exchange(tile_sums(True, gathered, members, (size, block)), ROW)
    states, summed_t, spread = call(
        state_kernel,
        (shape((nodes, width), F32), shape((width, nodes), F32), shape((members, nodes, size), BF16)),
        [VMEM] * 5,
    )(parts, inv_row, weight, driving, cotangent_scaled)
    blocks = exchange(spread, ROW)
    parts = exchange(tile_sums(False, blocks, sides, (block, size)), SIDE)
    factor = 1.0 / math.sqrt(nodes * members * col_devices)
    total = width + inputs
    adjoint, sums = call(
        functools.partial(grad_kernel, factor=factor),
        (shape((nodes, width), F32), shape((2 * total, width // 2), BF16)),
        [VMEM] * 7,
    )(parts, inv_wide, cotangent, weight, states, summed_t, features_t)
    piece = (2 * total // members, width // 2)
    parts = exchange(sums.reshape(members, *piece), ROW)
    spread = call(sum_kernel, shape((col_devices, *piece), BF16), [VMEM])(parts)
    parts = exchange(spread, COL)
    spread = call(sum_kernel, shape((members, *piece), BF16), [VMEM])(parts)
    sums = exchange(spread, ROW).reshape(2 * total, width // 2)
    weight_grad, input_grad = call(
        last_kernel, (shape((width, width), F32), shape((inputs, width), F32)), [VMEM]
    )(sums)
    return states, adjoint, weight_grad, input_grad


def solution(mesh):
    sizes = mesh.devices.shape
    fine = Mesh(
        mesh.devices.reshape(2, sizes[0] // 4, 2, 2, sizes[1] // 2),
        ("xl", "z", "core", "xh", "y"),
    )
    every = ROW + COL
    return jax.shard_map(
        body,
        mesh=fine,
        in_specs=(
            P(every, None),
            P(every, None),
            P(every, None),
            P(every),
            P(ROW, COL, None, None, None),
            P(ROW, COL, None),
            P(ROW, COL, None),
            P(ROW, COL, None),
            P(),
            P(),
        ),
        out_specs=(P(every, None), P(every, None), P(), P()),
        check_vma=False,
    )
```

```python
import functools
import math

import jax
import jax.numpy as jnp
from jax import lax
from jax.experimental import pallas as pl
from jax.experimental.pallas import tpu as pltpu
from jax.sharding import Mesh, PartitionSpec as P


HIGH = lax.Precision.HIGHEST
BF16 = jnp.bfloat16
F32 = jnp.float32
COL = ("xh", "y")
SIDE = ("core", "xh", "y")
ROW = ("xl", "z", "core")
UNROLL = 32
REST = 16
FIRST_MIB = 56
VMEM = pl.BlockSpec(memory_space=pltpu.VMEM)
ANY = pl.BlockSpec(memory_space=pl.ANY)
SMEM = pl.BlockSpec(memory_space=pltpu.SMEM)


def shape(dims, dtype):
    return jax.ShapeDtypeStruct(dims, dtype)


def summed_up(parts, first=0, step=1):
    total = parts[first].astype(F32)
    for q in range(first + step, parts.shape[0], step):
        total += parts[q].astype(F32)
    return total


def first_kernel(state, degrees, out):
    inverse = lax.rsqrt(degrees[...].astype(F32))
    scaled = (jnp.transpose(state[...]) * inverse).astype(BF16)
    half = out.shape[0] // 2
    size = out.shape[1]
    for q in range(half):
        out[q] = scaled[:size, :]
        out[half + q] = scaled[size:, :]


def pack_kernel(rows, cols, live, out):
    for q, x in enumerate((rows, cols)):
        out[q : q + 1, :] = x[...]
    count = jnp.sum(live[...].astype(F32), axis=1, keepdims=True)
    out[2:3, :] = jnp.broadcast_to(count, live.shape).astype(jnp.int32)


def prep_kernel(shared, values, degrees, features, input_map, cotangent, inv_row, inv_wide, driving, features_t, cotangent_scaled):
    inverse = lax.rsqrt(degrees[...].astype(F32))
    inv_row[...] = inverse
    wide = jnp.transpose(jnp.broadcast_to(inverse, inv_wide.shape))
    inv_wide[...] = wide
    features_t[...] = jnp.transpose(features[...])
    driving[...] = jnp.dot(
        features[...], input_map[...], precision=HIGH, preferred_element_type=F32
    )
    cotangent_scaled[...] = cotangent[...] * wide[:, :1]


def add_group(size, begin, places, start, count, values, forward, blocks, acc):
    spare = acc.shape[0] - 1
    products, slots = [], []
    for u in range(size):
        t = begin + u
        row, col = start + places[0, t], places[1, t]
        if forward:
            product = jnp.dot(blocks[row], values[t], preferred_element_type=F32)
        else:
            product = jnp.dot(values[t], blocks[col], preferred_element_type=F32)
        products.append(product)
        slots.append(jnp.where(t < count, col if forward else row, spare))
    for slot, product in zip(slots, products):
        acc[slot] += product


def tiles_kernel(core_ref, places, other_places, values, other_values, blocks, out, acc, held, sems, *, forward):
    core = core_ref[0]
    mine, theirs = places[2, 0], other_places[2, 0]
    step = blocks.shape[0] // 2 if forward else out.shape[0] // 2
    pieces = held.shape[0] // REST
    copies = []
    for j in range(pieces):
        part = pl.ds(j * REST, REST)
        copies.append(pltpu.make_async_copy(other_values.at[part], held.at[part], sems.at[j]))

        @pl.when(theirs > j * REST)
        def _(j=j):
            copies[j].start()

    acc[...] = jnp.zeros_like(acc)

    def own(size, first, g, carry):
        add_group(size, first + g * size, places, core * step, mine, values, forward, blocks, acc)
        return carry

    full = mine // UNROLL
    done = full * UNROLL
    lax.fori_loop(0, full, functools.partial(own, UNROLL, 0), 0)
    lax.fori_loop(0, (mine - done + REST - 1) // REST, functools.partial(own, REST, done), 0)
    for j in range(pieces):

        @pl.when(theirs > j * REST)
        def _(j=j):
            copies[j].wait()
            add_group(
                REST, j * REST, other_places, (1 - core) * step, theirs, held, forward, blocks, acc
            )

    out[...] = acc[0 : out.shape[0]].astype(BF16)


def state_kernel(parts, inv_row, weight, driving, cotangent_scaled, states, summed_t, out):
    total = jnp.concatenate([summed_up(parts, 0, 2), summed_up(parts, 1, 2)], axis=0)
    total = total * inv_row[...]
    summed_t[...] = total
    moved = jnp.dot(jnp.transpose(total), weight[...], precision=HIGH, preferred_element_type=F32)
    state = jnp.tanh(moved + driving[...])
    states[...] = state
    slopes = 1.0 - state * state
    scaled = (slopes * cotangent_scaled[...]).astype(BF16)
    size = out.shape[2]
    for q in range(out.shape[0]):
        out[q] = scaled[:, (q % 2) * size : (q % 2 + 1) * size]


def grad_kernel(
    parts, inv_wide, cotangent, weight, states, summed_t, features_t, adjoint, out, *, factor
):
    middle = parts.shape[0] // 2
    total = jnp.concatenate(
        [summed_up(parts.at[pl.ds(0, middle)]), summed_up(parts.at[pl.ds(middle, middle)])], axis=1
    )
    pulled = total * inv_wide[:, :1]
    moved = lax.dot_general(
        pulled, weight[...], (((1,), (1,)), ((), ())), precision=HIGH, preferred_element_type=F32
    )
    result = cotangent[...] + moved
    adjoint[...] = result
    state = states[...]
    masked = (1.0 - state * state) * result * factor
    weight_part = jnp.dot(summed_t[...], masked, precision=HIGH, preferred_element_type=F32)
    input_part = jnp.dot(features_t[...], masked, precision=HIGH, preferred_element_type=F32)
    half = out.shape[1]
    at = 0
    for side in range(2):
        for part in (weight_part, input_part):
            piece = part[:, side * half : (side + 1) * half]
            out[at : at + piece.shape[0], :] = piece.astype(out.dtype)
            at += piece.shape[0]


def sum_kernel(parts, out):
    total = summed_up(parts).astype(out.dtype)
    for q in range(out.shape[0]):
        out[q] = total


def last_kernel(sums, weight_grad, input_grad):
    half = sums.shape[1]
    at = 0
    for side in range(2):
        for out in (weight_grad, input_grad):
            out[:, side * half : (side + 1) * half] = sums[at : at + out.shape[0], :].astype(F32)
            at += out.shape[0]


def call(kernel, outs, specs, scratch=(), mib=12, flops=10**8, out_specs=None):
    return pl.pallas_call(
        kernel,
        out_shape=outs,
        in_specs=specs,
        out_specs=jax.tree.map(lambda _: VMEM, outs) if out_specs is None else out_specs,
        scratch_shapes=list(scratch),
        compiler_params=pltpu.CompilerParams(vmem_limit_bytes=mib * 2**20),
        cost_estimate=pl.CostEstimate(flops=flops, bytes_accessed=2**21, transcendentals=0),
    )


def swap(x):
    return lax.ppermute(x, "core", [(0, 1), (1, 0)])


def exchange(x, axes):
    return lax.all_to_all(x, axes, 0, 0, tiled=True)


def body(
    starting_state,
    features,
    cotangent,
    degrees,
    tile_values,
    tile_rows,
    tile_cols,
    tile_live,
    weight,
    input_map,
):
    values = tile_values[0, 0]
    nodes, width = starting_state.shape
    inputs = features.shape[1]
    members = lax.axis_size(ROW)
    col_devices = lax.axis_size(COL)
    sides = 2 * col_devices
    core = lax.axis_index("core").astype(jnp.int32).reshape(1)
    degree_row = degrees.reshape(1, nodes)
    slots, block = values.shape[:2]
    size = width // 2
    places = call(
        pack_kernel, shape((3, values.shape[0]), jnp.int32), [VMEM] * 3, mib=4
    )(tile_rows[0], tile_cols[0], tile_live[0])

    spread = call(
        first_kernel, shape((sides, size, nodes), BF16), [VMEM] * 2, mib=FIRST_MIB
    )(starting_state, degree_row)
    gathered = exchange(spread, SIDE)
    other_places, other_values = swap(places), swap(values)
    prep = call(
        prep_kernel,
        (
            shape((1, nodes), F32),
            shape((nodes, nodes), F32),
            shape((nodes, width), F32),
            shape((inputs, nodes), F32),
            shape((nodes, width), F32),
        ),
        [ANY] + [VMEM] * 5,
    )
    inv_row, inv_wide, driving, features_t, cotangent_scaled = prep(
        other_values, values, degree_row, features, input_map, cotangent
    )
    order = (core, places, other_places, values, other_values)

    def tile_sums(forward, blocks, count, dims):
        return call(
            functools.partial(tiles_kernel, forward=forward),
            shape((count, *dims), BF16),
            [SMEM] * 3 + [VMEM, ANY, VMEM],
            [
                pltpu.VMEM((count + 1, *dims), F32),
                pltpu.VMEM(values.shape, BF16),
                pltpu.SemaphoreType.DMA((slots // REST,)),
            ],
            mib=16,
            flops=4 * values.shape[0] * block * block * size,
        )(*order, blocks)

    parts = exchange(tile_sums(True, gathered, members, (size, block)), ROW)
    states, summed_t, spread = call(
        state_kernel,
        (shape((nodes, width), F32), shape((width, nodes), F32), shape((members, nodes, size), BF16)),
        [VMEM] * 5,
    )(parts, inv_row, weight, driving, cotangent_scaled)
    blocks = exchange(spread, ROW)
    parts = exchange(tile_sums(False, blocks, sides, (block, size)), SIDE)
    factor = 1.0 / math.sqrt(nodes * members * col_devices)
    total = width + inputs
    adjoint, sums = call(
        functools.partial(grad_kernel, factor=factor),
        (shape((nodes, width), F32), shape((2 * total, width // 2), BF16)),
        [VMEM] * 7,
    )(parts, inv_wide, cotangent, weight, states, summed_t, features_t)
    piece = (2 * total // members, width // 2)
    parts = exchange(sums.reshape(members, *piece), ROW)
    spread = call(sum_kernel, shape((col_devices, *piece), BF16), [VMEM])(parts)
    parts = exchange(spread, COL)
    spread = call(sum_kernel, shape((members, *piece), BF16), [VMEM])(parts)
    sums = exchange(spread, ROW).reshape(2 * total, width // 2)
    weight_grad, input_grad = call(
        last_kernel, (shape((width, width), F32), shape((inputs, width), F32)), [VMEM]
    )(sums)
    return states, adjoint, weight_grad, input_grad


def solution(mesh):
    sizes = mesh.devices.shape
    fine = Mesh(
        mesh.devices.reshape(2, sizes[0] // 4, 2, 2, sizes[1] // 2),
        ("xl", "z", "core", "xh", "y"),
    )
    every = ROW + COL
    return jax.shard_map(
        body,
        mesh=fine,
        in_specs=(
            P(every, None),
            P(every, None),
            P(every, None),
            P(every),
            P(ROW, COL, None, None, None),
            P(ROW, COL, None),
            P(ROW, COL, None),
            P(ROW, COL, None),
            P(),
            P(),
        ),
        out_specs=(P(every, None), P(every, None), P(), P()),
        check_vma=False,
    )
```

```python
import functools
import math

import jax
import jax.numpy as jnp
from jax import lax
from jax.experimental import pallas as pl
from jax.experimental.pallas import tpu as pltpu
from jax.sharding import Mesh, PartitionSpec as P


HIGH = lax.Precision.HIGHEST
BF16 = jnp.bfloat16
F32 = jnp.float32
COL = ("xh", "y")
SIDE = ("xh", "y", "core")
ROW = ("xl", "z", "core")
UNROLL = 32
REST = 16
FIRST_MIB = 56
VMEM = pl.BlockSpec(memory_space=pltpu.VMEM)
ANY = pl.BlockSpec(memory_space=pl.ANY)
SMEM = pl.BlockSpec(memory_space=pltpu.SMEM)


def shape(dims, dtype):
    return jax.ShapeDtypeStruct(dims, dtype)


def summed_up(parts, first=0, step=1):
    total = parts[first].astype(F32)
    for q in range(first + step, parts.shape[0], step):
        total += parts[q].astype(F32)
    return total


def first_kernel(state, degrees, out):
    inverse = lax.rsqrt(degrees[...].astype(F32))
    scaled = (jnp.transpose(state[...]) * inverse).astype(BF16)
    size = out.shape[1]
    for q in range(out.shape[0]):
        out[q] = scaled[(q % 2) * size : (q % 2 + 1) * size, :]


def pack_kernel(rows, cols, live, out):
    for q, x in enumerate((rows, cols)):
        out[q : q + 1, :] = x[...]
    count = jnp.sum(live[...].astype(F32), axis=1, keepdims=True)
    out[2:3, :] = jnp.broadcast_to(count, live.shape).astype(jnp.int32)


def prep_kernel(shared, values, degrees, features, input_map, cotangent, inv_row, inv_wide, driving, features_t, cotangent_scaled):
    inverse = lax.rsqrt(degrees[...].astype(F32))
    inv_row[...] = inverse
    wide = jnp.transpose(jnp.broadcast_to(inverse, inv_wide.shape))
    inv_wide[...] = wide
    features_t[...] = jnp.transpose(features[...])
    driving[...] = jnp.dot(
        features[...], input_map[...], precision=HIGH, preferred_element_type=F32
    )
    cotangent_scaled[...] = cotangent[...] * wide[:, :1]


def add_group(size, begin, places, side, count, values, forward, blocks, acc):
    spare = acc.shape[0] - 1
    products, slots = [], []
    for u in range(size):
        t = begin + u
        row, col = 2 * places[0, t] + side, places[1, t]
        if forward:
            product = jnp.dot(blocks[row], values[t], preferred_element_type=F32)
        else:
            product = jnp.dot(values[t], blocks[col], preferred_element_type=F32)
        products.append(product)
        slots.append(jnp.where(t < count, col if forward else row, spare))
    for slot, product in zip(slots, products):
        acc[slot] += product


def tiles_kernel(core_ref, places, other_places, values, other_values, blocks, out, acc, held, sems, *, forward):
    core = core_ref[0]
    mine, theirs = places[2, 0], other_places[2, 0]
    pieces = held.shape[0] // REST
    copies = []
    for j in range(pieces):
        part = pl.ds(j * REST, REST)
        copies.append(pltpu.make_async_copy(other_values.at[part], held.at[part], sems.at[j]))

        @pl.when(theirs > j * REST)
        def _(j=j):
            copies[j].start()

    acc[...] = jnp.zeros_like(acc)

    def own(size, first, g, carry):
        add_group(size, first + g * size, places, core, mine, values, forward, blocks, acc)
        return carry

    full = mine // UNROLL
    done = full * UNROLL
    lax.fori_loop(0, full, functools.partial(own, UNROLL, 0), 0)
    lax.fori_loop(0, (mine - done + REST - 1) // REST, functools.partial(own, REST, done), 0)
    for j in range(pieces):

        @pl.when(theirs > j * REST)
        def _(j=j):
            copies[j].wait()
            add_group(
                REST, j * REST, other_places, 1 - core, theirs, held, forward, blocks, acc
            )

    out[...] = acc[0 : out.shape[0]].astype(BF16)


def state_kernel(parts, inv_row, weight, driving, cotangent_scaled, states, summed_t, out):
    total = jnp.concatenate([summed_up(parts, 0, 2), summed_up(parts, 1, 2)], axis=0)
    total = total * inv_row[...]
    summed_t[...] = total
    moved = jnp.dot(jnp.transpose(total), weight[...], precision=HIGH, preferred_element_type=F32)
    state = jnp.tanh(moved + driving[...])
    states[...] = state
    slopes = 1.0 - state * state
    scaled = (slopes * cotangent_scaled[...]).astype(BF16)
    size = out.shape[2]
    for q in range(out.shape[0]):
        out[q] = scaled[:, (q % 2) * size : (q % 2 + 1) * size]


def grad_kernel(
    parts, inv_wide, cotangent, weight, states, summed_t, features_t, adjoint, out, *, factor
):
    total = jnp.concatenate([summed_up(parts, 0, 2), summed_up(parts, 1, 2)], axis=1)
    pulled = total * inv_wide[:, :1]
    moved = lax.dot_general(
        pulled, weight[...], (((1,), (1,)), ((), ())), precision=HIGH, preferred_element_type=F32
    )
    result = cotangent[...] + moved
    adjoint[...] = result
    state = states[...]
    masked = (1.0 - state * state) * result * factor
    weight_part = jnp.dot(summed_t[...], masked, precision=HIGH, preferred_element_type=F32)
    input_part = jnp.dot(features_t[...], masked, precision=HIGH, preferred_element_type=F32)
    half = out.shape[1]
    at = 0
    for side in range(2):
        for part in (weight_part, input_part):
            piece = part[:, side * half : (side + 1) * half]
            out[at : at + piece.shape[0], :] = piece.astype(out.dtype)
            at += piece.shape[0]


def sum_kernel(parts, out):
    total = summed_up(parts).astype(out.dtype)
    for q in range(out.shape[0]):
        out[q] = total


def last_kernel(sums, weight_grad, input_grad):
    half = sums.shape[1]
    at = 0
    for side in range(2):
        for out in (weight_grad, input_grad):
            out[:, side * half : (side + 1) * half] = sums[at : at + out.shape[0], :].astype(F32)
            at += out.shape[0]


def call(kernel, outs, specs, scratch=(), mib=12, flops=10**8, out_specs=None):
    return pl.pallas_call(
        kernel,
        out_shape=outs,
        in_specs=specs,
        out_specs=jax.tree.map(lambda _: VMEM, outs) if out_specs is None else out_specs,
        scratch_shapes=list(scratch),
        compiler_params=pltpu.CompilerParams(vmem_limit_bytes=mib * 2**20),
        cost_estimate=pl.CostEstimate(flops=flops, bytes_accessed=2**21, transcendentals=0),
    )


def swap(x):
    return lax.ppermute(x, "core", [(0, 1), (1, 0)])


def exchange(x, axes):
    return lax.all_to_all(x, axes, 0, 0, tiled=True)


def body(
    starting_state,
    features,
    cotangent,
    degrees,
    tile_values,
    tile_rows,
    tile_cols,
    tile_live,
    weight,
    input_map,
):
    values = tile_values[0, 0]
    nodes, width = starting_state.shape
    inputs = features.shape[1]
    members = lax.axis_size(ROW)
    col_devices = lax.axis_size(COL)
    sides = 2 * col_devices
    core = lax.axis_index("core").astype(jnp.int32).reshape(1)
    degree_row = degrees.reshape(1, nodes)
    slots, block = values.shape[:2]
    size = width // 2
    places = call(
        pack_kernel, shape((3, values.shape[0]), jnp.int32), [VMEM] * 3, mib=4
    )(tile_rows[0], tile_cols[0], tile_live[0])

    spread = call(
        first_kernel, shape((sides, size, nodes), BF16), [VMEM] * 2, mib=FIRST_MIB
    )(starting_state, degree_row)
    gathered = exchange(spread, SIDE)
    other_places, other_values = swap(places), swap(values)
    prep = call(
        prep_kernel,
        (
            shape((1, nodes), F32),
            shape((nodes, nodes), F32),
            shape((nodes, width), F32),
            shape((inputs, nodes), F32),
            shape((nodes, width), F32),
        ),
        [ANY] + [VMEM] * 5,
    )
    inv_row, inv_wide, driving, features_t, cotangent_scaled = prep(
        other_values, values, degree_row, features, input_map, cotangent
    )
    order = (core, places, other_places, values, other_values)

    def tile_sums(forward, blocks, count, dims):
        return call(
            functools.partial(tiles_kernel, forward=forward),
            shape((count, *dims), BF16),
            [SMEM] * 3 + [VMEM, ANY, VMEM],
            [
                pltpu.VMEM((count + 1, *dims), F32),
                pltpu.VMEM(values.shape, BF16),
                pltpu.SemaphoreType.DMA((slots // REST,)),
            ],
            mib=16,
            flops=4 * values.shape[0] * block * block * size,
        )(*order, blocks)

    parts = exchange(tile_sums(True, gathered, members, (size, block)), ROW)
    states, summed_t, spread = call(
        state_kernel,
        (shape((nodes, width), F32), shape((width, nodes), F32), shape((members, nodes, size), BF16)),
        [VMEM] * 5,
    )(parts, inv_row, weight, driving, cotangent_scaled)
    blocks = exchange(spread, ROW)
    parts = exchange(tile_sums(False, blocks, sides, (block, size)), SIDE)
    factor = 1.0 / math.sqrt(nodes * members * col_devices)
    total = width + inputs
    adjoint, sums = call(
        functools.partial(grad_kernel, factor=factor),
        (shape((nodes, width), F32), shape((2 * total, width // 2), BF16)),
        [VMEM] * 7,
    )(parts, inv_wide, cotangent, weight, states, summed_t, features_t)
    piece = (2 * total // members, width // 2)
    parts = exchange(sums.reshape(members, *piece), ROW)
    spread = call(sum_kernel, shape((col_devices, *piece), BF16), [VMEM])(parts)
    parts = exchange(spread, COL)
    spread = call(sum_kernel, shape((members, *piece), BF16), [VMEM])(parts)
    sums = exchange(spread, ROW).reshape(2 * total, width // 2)
    weight_grad, input_grad = call(
        last_kernel, (shape((width, width), F32), shape((inputs, width), F32)), [VMEM]
    )(sums)
    return states, adjoint, weight_grad, input_grad


def solution(mesh):
    sizes = mesh.devices.shape
    fine = Mesh(
        mesh.devices.reshape(2, sizes[0] // 4, 2, 2, sizes[1] // 2),
        ("xl", "z", "core", "xh", "y"),
    )
    every = ROW + COL
    return jax.shard_map(
        body,
        mesh=fine,
        in_specs=(
            P(every, None),
            P(every, None),
            P(every, None),
            P(every),
            P(ROW, COL, None, None, None),
            P(ROW, COL, None),
            P(ROW, COL, None),
            P(ROW, COL, None),
            P(),
            P(),
        ),
        out_specs=(P(every, None), P(every, None), P(), P()),
        check_vma=False,
    )
```
